256 devices in a mesh: gx: 8 (over x, core), gy: 8 (over z), wa: 4 (over y).
Axes of the slice: x: 4, y: 4, z: 8, core: 2. Of those that a mesh axis runs over, the one named last changes fastest.
Arguments:
- velocity: float32 [3, 256, 512, 512], P(None, 'gx', 'gy', 'wa'), may hold values from -70 to 70, as said below
- lengths: int32 [8, 8, 4, 2048], P('gx', 'gy', 'wa'), may hold values from 16 to 128
- destinations: int32 [8, 8, 4, 2048, 1], P('gx', 'gy', 'wa'), may hold values from 0 to 63; in each aligned block of 2048 rows (0 to 2047, 2048 to 4095, ..., all dimensions but the last counted through in order) at most 64 rows name the same one
Outputs:
- received: float32 [64, 4, 3, 64, 64, 128], P(('gx', 'gy'), 'wa')
The draws below stay inside these ranges and needn't reach their ends.
Inputs may be any that keep to these rules, and one draw needn't show every extreme that they name: `velocity`: finite values; the amplitude varies over the grid. `destinations`: in every draw no device sends more than 64 blocks to one writer, and some device sends exactly 64 to one writer.
All inputs are finite; a program needn't handle non-finite values.
Results may differ from the reference program's by a relative error of at most 0.0003.
Values sent between devices are 32-bit elements; how exact they have to be, the bound alone decides.
No kernel may reach another device: no remote copies, remote signals or barrier semaphores. Data moves between devices by JAX's collectives and lax.ppermute only.
A program may use at most 128 MiB of HBM per device.

```python
import math
import jax
import jax.numpy as jnp
import numpy as np
from jax import lax

CX = 32
CY = 64
CZ = 128
COMP = 3
BY = 8
BZ = 16
COEF = 128
NBLK = 2048
WRITERS = 64
CAP = 64
NX = 256
NY = 512
NZ = 512
N_GX = 8
N_GY = 8
N_WA = 4


def draw_velocity(key, part):
    xs = jnp.arange(NX, dtype=jnp.float32)[:, None, None] / NX
    ys = jnp.arange(NY, dtype=jnp.float32)[None, :, None] / NY
    noise = jax.random.truncated_normal(key, -6.0, 6.0, (COMP, NX, NY, NZ), jnp.float32)
    amplitude = jnp.exp(jnp.log(10.0) * 0.5 * (xs + ys))
    return amplitude * noise


def place_ends(entries, rng, least, high):
    shape = entries.shape
    spot = [jax.random.randint(jax.random.fold_in(rng, axis), (), 0, shape[axis]) for axis in range(len(shape))]
    entries = entries.at[tuple(spot)].set(least)
    longest = shape.index(max(shape))
    spot[longest] = (spot[longest] + 1) % shape[longest]
    return entries.at[tuple(spot)].set(high)


def shared_out(own_key, own, number, rows, number_of, top, bound, skew):
    sequence = jax.random.permutation(own_key, number_of)
    crowded, usual = load_shares(number_of, rows * top, bound, skew, True), load_shares(number_of, rows * top, bound, skew, False)
    places = jnp.arange(number_of)

    def named(tallies, turn):
        used = int((tallies > 0).sum())
        fixed = max(1, used // 4)
        passed = fixed + (places - fixed + turn * (used - fixed)) % max(1, number_of - fixed)
        return jnp.zeros((number_of,), jnp.int32).at[sequence[jnp.where(places < fixed, places, passed)]].set(jnp.asarray(tallies, jnp.int32))

    tallies = jnp.where(number % 4 == 0, named(crowded, number // 4), named(usual, number - number // 4 - 1))
    mixed = jax.random.permutation(jax.random.fold_in(own, 3), number_of)
    giver, receiver = mixed[0:number_of // 2 * 2:2], mixed[1:number_of // 2 * 2:2]
    room = jnp.minimum(tallies[giver] - 1, bound - tallies[receiver]) // 2
    room = jnp.where((giver == sequence[0]) | (receiver == sequence[0]) | (tallies[receiver] == 0), 0, jnp.maximum(room, 0))
    passed = jax.random.randint(jax.random.fold_in(own, 4), (number_of // 2,), 0, 1 << 20) % (room + 1)
    tallies = tallies.at[giver].add(-passed).at[receiver].add(passed)
    members = jnp.searchsorted(jnp.cumsum(tallies), jnp.arange(rows * top), side="right").astype(jnp.int32)
    grid = members.reshape(top, rows).T
    grid = grid[jax.random.permutation(jax.random.fold_in(own, 1), rows)]
    turn = jax.random.randint(jax.random.fold_in(own, 2), (rows, 1), 0, top)
    return jnp.take_along_axis(grid, (jnp.arange(top)[None, :] + turn) % top, axis=1)


def load_shares(count, total, reach, lean, full):
    weights = [(1 << 20) // math.isqrt(standing ** lean) + 1 for standing in range(1, count + 1)]
    largest = reach if full else min(reach, max(-(-total // count), total * weights[0] // sum(weights)))
    least = 1 if total - largest >= count - 1 else 0
    given, spare = [largest] + [least] * (count - 1), total - largest - least * (count - 1)
    while spare > 0:
        free = [i for i in range(1, count) if given[i] < largest] or [i for i in range(1, count) if given[i] < reach]
        pool, budget = sum([weights[i] for i in free]), spare
        for i in free:
            more = min(reach - given[i], max(1, budget * weights[i] // pool), spare)
            given[i] = given[i] + more
            spare = spare - more
    return np.array(given)


def setup_inputs(seed: int = 0) -> dict:
    key_list = jax.random.split(jax.random.key(seed), 4)
    velocity = draw_velocity(jax.random.fold_in(key_list[3], 71), 0)
    lengths = place_ends(jax.random.randint(key_list[1], (N_GX, N_GY, N_WA, NBLK), 16, COEF + 1), jax.random.fold_in(key_list[1], 1), 16, COEF).astype(jnp.int32)
    destinations_keys = jax.random.split(jax.random.fold_in(key_list[2], 1), N_GX * N_GY * N_WA * NBLK // NBLK)
    destinations_turns = jax.random.permutation(jax.random.fold_in(key_list[2], 3), N_GX * N_GY * N_WA * NBLK // NBLK)
    destinations = jax.vmap(lambda own, number: shared_out(jax.random.fold_in(key_list[2], 2), own, number, NBLK, WRITERS, 1, CAP, 2))(destinations_keys, destinations_turns).reshape((N_GX, N_GY, N_WA, NBLK, 1))
    return dict(velocity=velocity, lengths=lengths, destinations=destinations)


def dct_table(count):
    freqs = jnp.arange(count, dtype=jnp.float32)[:, None]
    points = jnp.arange(count, dtype=jnp.float32)[None, :]
    table = jnp.cos(jnp.pi * (points + 0.5) * freqs / count) * jnp.sqrt(2.0 / count)
    return jnp.where(freqs == 0.0, table * jnp.sqrt(0.5), table)

def curl_field(padded):

    def along_x(component):
        return (padded[component, 2:, 1:-1, 1:-1] - padded[component, :-2, 1:-1, 1:-1]) * 0.5

    def along_y(component):
        return (padded[component, 1:-1, 2:, 1:-1] - padded[component, 1:-1, :-2, 1:-1]) * 0.5

    def along_z(component):
        return (padded[component, 1:-1, 1:-1, 2:] - padded[component, 1:-1, 1:-1, :-2]) * 0.5
    first = along_y(2) - along_z(1)
    second = along_z(0) - along_x(2)
    third = along_x(1) - along_y(0)
    return jnp.stack([first, second, third])

def place_blocks(scaled, lens, targets):
    onehot = (targets[:, None] == jnp.arange(WRITERS, dtype=jnp.int32)[None, :]).astype(jnp.int32)
    before = jnp.cumsum(onehot, axis=0) - onehot
    ranking = lax.optimization_barrier(jnp.sum(before * onehot, axis=1))
    slot_index = (targets * CAP + ranking).astype(jnp.int32)
    buffer = jnp.zeros((WRITERS * CAP, COMP, COEF), jnp.float32)
    buffer = buffer.at[slot_index].set(scaled)
    return buffer.reshape(WRITERS, CAP, COMP, COEF)

def reference(velocity, lengths, destinations):
    padded = jnp.pad(velocity, ((0, 0), (1, 1), (1, 1), (1, 1)), mode='wrap')
    curl = curl_field(padded)
    total = jnp.sum(curl * curl)
    rms = jnp.sqrt(total / (COMP * NX * NY * NZ) + 1e-06)
    kron_table = jnp.kron(dct_table(BY), dct_table(BZ))
    grouped = curl.reshape(COMP, N_GX, CX, N_GY, CY // BY, BY, N_WA, CZ // BZ, BZ)
    grouped = grouped.transpose(1, 3, 6, 2, 4, 7, 0, 5, 8)
    blocks = grouped.reshape(-1, COEF)
    coeffs = jnp.dot(blocks, kron_table.T, precision=lax.Precision.HIGHEST, preferred_element_type=jnp.float32)
    coeffs = coeffs.reshape(N_GX * N_GY * N_WA, NBLK, COMP, COEF)
    freqs = jnp.arange(COEF, dtype=jnp.int32)
    lens = lengths.reshape(N_GX * N_GY * N_WA, NBLK)
    keep = (freqs[None, None, None, :] < lens[:, :, None, None]).astype(jnp.float32)
    scaled = coeffs * keep / rms
    targets = destinations.reshape(N_GX * N_GY * N_WA, NBLK)
    buffers = jax.vmap(place_blocks)(scaled, lens, targets)
    buffers = buffers.reshape(WRITERS, N_WA, WRITERS, CAP, COMP, COEF)
    return buffers.transpose(2, 1, 4, 0, 3, 5)
```

```python
import functools

import jax
import jax.numpy as jnp
import numpy as np
from jax import lax
from jax.experimental import pallas as pl
from jax.experimental.pallas import tpu as pltpu
from jax.sharding import PartitionSpec as P

BY = 8
BZ = 16
LANES = 128
COMP = 3
CX = 32
CY = 64
NBLK = 2048
WRITERS = 64
CAP = 64
ROWS = 45
CELLS = 256 * 512 * 512 * 3
G = ("gx", "gy")


def span_of(rows):
    return -(-(COMP * rows + 1) // 8) * 8


def dct_np(n):
    k = np.arange(n, dtype=np.float64)[:, None]
    j = np.arange(n, dtype=np.float64)[None, :]
    t = np.sqrt(2.0 / n) * np.cos(np.pi * (j + 0.5) * k / n)
    t[0] *= np.sqrt(0.5)
    return t


def table_np():
    k = (0.5 * np.kron(dct_np(BY), dct_np(BZ)).T).astype(np.float32)
    high = k.astype(jnp.bfloat16)
    low = (k - high.astype(np.float32)).astype(jnp.bfloat16)
    top = np.concatenate([high, low], axis=1)
    bottom = np.concatenate([high, np.zeros_like(low)], axis=1)
    return np.concatenate([top, bottom], axis=0)


def iota(shape, dim):
    return lax.broadcasted_iota(jnp.int32, shape, dim)


def faces_kernel(vel, xlo, xhi, ylo, yhi, zt):
    plane = CY
    comp = CX * CY
    for n, c in enumerate((1, 2)):
        xlo[n * plane : (n + 1) * plane] = vel[c * comp : c * comp + plane]
        xhi[n * plane : (n + 1) * plane] = vel[(c + 1) * comp - plane : (c + 1) * comp]
    for n, c in enumerate((0, 2)):
        ylo[n * CX : (n + 1) * CX] = vel[pl.ds(c * comp, CX, stride=plane)]
        yhi[n * CX : (n + 1) * CX] = vel[pl.ds(c * comp + plane - 1, CX, stride=plane)]
    lane = iota((CY, LANES), 1)
    t = jnp.zeros((CY, LANES), jnp.float32)
    for k in range(2 * CX):
        f = vel[k * plane : (k + 1) * plane]
        t = jnp.where((lane >> 1) == k, pltpu.roll(f, (2 * k + 1) % LANES, 1), t)
    zt[...] = t


def faces(vel2):
    f32 = jnp.float32
    return pl.pallas_call(
        faces_kernel,
        out_shape=[
            jax.ShapeDtypeStruct((2 * CY, LANES), f32),
            jax.ShapeDtypeStruct((2 * CY, LANES), f32),
            jax.ShapeDtypeStruct((2 * CX, LANES), f32),
            jax.ShapeDtypeStruct((2 * CX, LANES), f32),
            jax.ShapeDtypeStruct((CY, LANES), f32),
        ],
        cost_estimate=pl.CostEstimate(flops=4_000_000, bytes_accessed=3_500_000, transcendentals=0),
        name="faces",
    )(vel2)


def index_kernel(tgt, length, words, wide, head):
    chunks = NBLK // LANES
    t = tgt[...]
    ln = length[...]
    row = iota((WRITERS, LANES), 0)
    before = (iota((LANES, LANES), 0) < iota((LANES, LANES), 1)).astype(jnp.bfloat16)
    ones = jnp.ones((LANES, LANES), jnp.bfloat16)
    rhs = jnp.concatenate([before, ones], axis=1)
    hits, weighted = [], []
    for r in range(chunks):
        hit = t[r : r + 1, :] == row
        hits.append(hit)
        weighted.append(jnp.where(hit, ln[r : r + 1, :], 0).astype(jnp.float32).astype(jnp.bfloat16))
    counted = [jnp.where(h, 1.0, 0.0).astype(jnp.bfloat16) for h in hits]
    nt = (((1,), (1,)), ((), ()))
    base_l = jnp.zeros((WRITERS, LANES), jnp.float32)
    base_c = jnp.zeros((WRITERS, LANES), jnp.float32)
    lens = jnp.zeros((WRITERS, LANES), jnp.float32)
    starts = []
    for r in range(chunks):
        sums_l = jnp.dot(weighted[r], rhs, preferred_element_type=jnp.float32)
        sums_c = jnp.dot(counted[r], rhs, preferred_element_type=jnp.float32)
        start = jnp.where(hits[r], sums_l[:, :LANES] + base_l, 0.0)
        rank = jnp.where(hits[r], sums_c[:, :LANES] + base_c, 0.0)
        starts.append(jnp.sum(start, axis=0, keepdims=True))
        slot = jnp.sum(rank, axis=0, keepdims=True).astype(jnp.int32)
        at = jnp.where(slot == iota((LANES, LANES), 0), 1.0, 0.0).astype(jnp.bfloat16)
        lens += lax.dot_general(weighted[r], at, nt, preferred_element_type=jnp.float32)
        base_l += sums_l[:, LANES:]
        base_c += sums_c[:, LANES:]
    start = jnp.concatenate(starts, axis=0).astype(jnp.int32)
    first = start >> 7
    shift = start & (LANES - 1)
    over = jnp.maximum(shift + ln - LANES, 0)
    for out, rows in ((words, ROWS), (wide, CAP)):
        addr = t * span_of(rows) + COMP * jnp.minimum(first, rows - 1)
        lo = jnp.where(first < rows, shift, LANES)
        second = jnp.where(first + 1 < rows, over, 0)
        out[...] = addr + (lo << 14) + (second << 22)
    full = jnp.max(base_l, axis=0, keepdims=True)
    spill = jnp.where(full > ROWS * LANES, 1.0, 0.0)
    lane = iota((WRITERS, LANES), 1)
    head[...] = jnp.where(lane < CAP, lens, jnp.where(lane == CAP + 1, spill, 0.0))


def index(targets, lens):
    i32 = jnp.int32
    return pl.pallas_call(
        index_kernel,
        out_shape=[
            jax.ShapeDtypeStruct((NBLK // LANES, LANES), i32),
            jax.ShapeDtypeStruct((NBLK // LANES, LANES), i32),
            jax.ShapeDtypeStruct((WRITERS, LANES), jnp.float32),
        ],
        cost_estimate=pl.CostEstimate(flops=20_000_000, bytes_accessed=100_000, transcendentals=0),
        name="index",
    )(targets, lens)


PLANES = 4


def transform_kernel(vel, xprev, xnext, yprev, ynext, zprev, znext, table, out, sq, ends, scratch, blocks):
    step = pl.program_id(0)
    comp = CX * CY
    lane = iota((CY, LANES), 1)
    row = iota((CY, LANES), 0)

    @pl.when(step == 0)
    def _():
        ends[...] = jnp.where(
            (lane & 1) == 0, pltpu.roll(znext[...], LANES - 1, 1), pltpu.roll(zprev[...], 1, 1)
        )
        sq[...] = jnp.zeros_like(sq)

    first, last = lane == 0, lane == LANES - 1
    granule = iota((8, LANES), 1) >> 4

    def plane_of(c, x):
        return vel[pl.ds(pl.multiple_of(c * comp + x * CY, CY), CY)]

    def along_x(c, x, n):
        low = jnp.maximum(x - 1, 0)
        high = jnp.minimum(x + 1, CX - 1)
        below = jnp.where(x == 0, xprev[n * CY : (n + 1) * CY], plane_of(c, low))
        above = jnp.where(x == CX - 1, xnext[n * CY : (n + 1) * CY], plane_of(c, high))
        return above - below

    def along_y(f, x, n):
        above = jnp.where(row == CY - 1, ynext[pl.ds(n * CX + x, CY, stride=0)], pltpu.roll(f, CY - 1, 0))
        below = jnp.where(row == 0, yprev[pl.ds(n * CX + x, CY, stride=0)], pltpu.roll(f, 1, 0))
        return above - below

    def along_z(f, c, x):
        edge = pltpu.roll(ends[...], LANES - 1 - 2 * (c * CX + x), 1)
        above = jnp.where(last, edge, pltpu.roll(f, LANES - 1, 1))
        below = jnp.where(first, edge, pltpu.roll(f, 1, 1))
        return above - below

    total = jnp.zeros((8, LANES), jnp.float32)
    for p in range(PLANES):
        x = step * PLANES + p
        u, v, w = plane_of(0, x), plane_of(1, x), plane_of(2, x)
        curl = (
            along_y(w, x, 1) - along_z(v, 1, x),
            along_z(u, 0, x) - along_x(2, x, 1),
            along_x(1, x, 0) - along_y(u, x, 0),
        )
        for c in range(COMP):
            f = curl[c]
            square = f * f
            for i in range(CY // 8):
                total += square[i * 8 : (i + 1) * 8]
            at = (p * COMP + c) * CY
            scratch[at : at + CY] = f
            tiles = [scratch[pl.ds(at + y, 8, stride=8)] for y in range(8)]
            for b in (4, 2, 1):
                low = (granule & b) == 0
                fresh = list(tiles)
                for j in range(8):
                    if j & b == 0:
                        one, two = tiles[j], tiles[j | b]
                        fresh[j] = jnp.where(low, one, pltpu.roll(two, 16 * b, 1))
                        fresh[j | b] = jnp.where(low, pltpu.roll(one, LANES - 16 * b, 1), two)
                tiles = fresh
            whole = jnp.concatenate(tiles, axis=0)
            high = whole.astype(jnp.bfloat16)
            low = (whole - high.astype(jnp.float32)).astype(jnp.bfloat16)
            blocks[at : at + CY, :LANES] = high
            blocks[at : at + CY, LANES:] = low
    sq[...] += total
    for p in range(PLANES):
        at = p * COMP * CY
        both = jnp.dot(
            blocks[at : at + COMP * CY], table[...], preferred_element_type=jnp.float32
        )
        coeffs = both[:, :LANES] + both[:, LANES:]
        for c in range(COMP):
            for zb in range(8):
                piece = coeffs[c * CY + zb * 8 : c * CY + zb * 8 + 8]
                out[pl.ds(COMP * (p * CY + zb * 8) + c, 8, stride=COMP)] = piece


def transform(vel2, xprev, xnext, yprev, ynext, zprev, znext):
    table = jnp.asarray(table_np())
    rows = PLANES * COMP * CY
    whole = lambda a: pl.BlockSpec(a.shape, lambda i: (0, 0))
    args = (vel2, xprev, xnext, yprev, ynext, zprev, znext, table)
    return pl.pallas_call(
        transform_kernel,
        grid=(CX // PLANES,),
        in_specs=[whole(a) for a in args],
        out_specs=[
            pl.BlockSpec((rows, LANES), lambda i: (i, 0)),
            pl.BlockSpec((8, LANES), lambda i: (0, 0)),
        ],
        out_shape=[
            jax.ShapeDtypeStruct((COMP * NBLK, LANES), jnp.float32),
            jax.ShapeDtypeStruct((8, LANES), jnp.float32),
        ],
        scratch_shapes=[
            pltpu.VMEM((CY, LANES), jnp.float32),
            pltpu.VMEM((rows, LANES), jnp.float32),
            pltpu.VMEM((rows, 2 * LANES), jnp.bfloat16),
        ],
        cost_estimate=pl.CostEstimate(
            flops=2 * COMP * NBLK * 256 * 256, bytes_accessed=6_500_000, transcendentals=0
        ),
        name="transform",
    )(*args)


PACK_STEPS = 4


def pack_kernel(limit, words, coeffs, out):
    step = pl.program_id(0)
    per = NBLK // LANES // PACK_STEPS
    lane = iota((COMP, LANES), 1)

    def body(r, carry):
        at = step * per + r
        for j in range(LANES):
            plane, yb, zb = j // CY, (j % CY) // 8, j % 8
            word = words[at, j]
            addr = word & 16383
            lo = (word >> 14) & 255
            second = word >> 22
            source = COMP * (plane * CY + zb * 8 + yb)
            value = coeffs[pl.ds(r * (COMP * LANES) + source, COMP)]
            turned = pltpu.roll(value, lo & (LANES - 1), 1)
            pltpu.store(out.at[pl.ds(addr, COMP)], turned, mask=lane >= lo)
            nxt = jnp.minimum(addr + COMP, limit)
            pltpu.store(out.at[pl.ds(nxt, COMP)], turned, mask=lane < second)
        return carry

    lax.fori_loop(0, per, body, 0)


def pack(words, coeffs, rows):
    span = span_of(rows)
    block = COMP * NBLK // PACK_STEPS
    return pl.pallas_call(
        functools.partial(pack_kernel, WRITERS * span - COMP),
        grid=(PACK_STEPS,),
        in_specs=[
            pl.BlockSpec(memory_space=pltpu.SMEM),
            pl.BlockSpec((block, LANES), lambda i: (i, 0)),
        ],
        out_specs=pl.BlockSpec((WRITERS * span, LANES), lambda i: (0, 0)),
        out_shape=jax.ShapeDtypeStruct((WRITERS * span, LANES), jnp.float32),
        cost_estimate=pl.CostEstimate(
            flops=200_000_000, bytes_accessed=8_000_000, transcendentals=0
        ),
        name=f"pack{rows}",
    )(words, coeffs)


def decode_kernel(head, words, scale, spill):
    h = head[...]
    lane = iota((WRITERS, LANES), 1)
    lens = jnp.where(lane < CAP, h, 0.0)
    before = (iota((LANES, LANES), 0) < iota((LANES, LANES), 1)).astype(jnp.bfloat16)
    start = jnp.dot(lens.astype(jnp.bfloat16), before, preferred_element_type=jnp.float32)
    start = start.astype(jnp.int32)
    words[...] = (
        COMP * (start >> 7) + ((start & (LANES - 1)) << 8) + (lens.astype(jnp.int32) << 16)
    )
    total = jnp.sum(jnp.where(lane == CAP, h, 0.0), keepdims=True)
    rms = jnp.sqrt(total * (1.0 / CELLS) + 1e-6)
    scale[...] = jnp.broadcast_to(1.0 / rms, scale.shape)
    flag = jnp.max(jnp.where(lane == CAP + 1, h, 0.0), keepdims=True)
    spill[...] = jnp.broadcast_to(flag, spill.shape).astype(jnp.int32)


def decode(head):
    return pl.pallas_call(
        decode_kernel,
        out_shape=[
            jax.ShapeDtypeStruct((WRITERS, LANES), jnp.int32),
            jax.ShapeDtypeStruct((8, LANES), jnp.float32),
            jax.ShapeDtypeStruct((8, LANES), jnp.int32),
        ],
        name="decode",
    )(head)


SOURCES = 8


def unpack_kernel(span, words, scale, recv, out):
    step = pl.program_id(0)
    lane = iota((COMP, LANES), 1)
    factor = scale[0:COMP, :]
    flat = out.reshape(COMP * SOURCES * CAP, LANES)
    limit = SOURCES * span - COMP

    def body(s, carry):
        base = s * span
        for q in range(CAP):
            word = words[step * SOURCES + s, q]
            lo = (word >> 8) & 255
            count = word >> 16
            at = jnp.minimum(base + (word & 255), limit)
            one = recv[pl.ds(at, COMP)]
            two = recv[pl.ds(jnp.minimum(at + COMP, limit), COMP)]
            both = jnp.where(lane >= lo, one, two)
            turned = pltpu.roll(both, (LANES - lo) & (LANES - 1), 1)
            value = jnp.where(lane < count, turned * factor, 0.0)
            flat[pl.ds(s * CAP + q, COMP, stride=SOURCES * CAP)] = value
        return carry

    lax.fori_loop(0, SOURCES, body, 0)


def unpack(words, scale, recv, rows):
    span = span_of(rows)
    return pl.pallas_call(
        functools.partial(unpack_kernel, span),
        grid=(WRITERS // SOURCES,),
        in_specs=[
            pl.BlockSpec(memory_space=pltpu.SMEM),
            pl.BlockSpec((8, LANES), lambda i: (0, 0)),
            pl.BlockSpec((SOURCES * span, LANES), lambda i: (i, 0)),
        ],
        out_specs=pl.BlockSpec((COMP, SOURCES * CAP, LANES), lambda i: (0, i, 0)),
        out_shape=jax.ShapeDtypeStruct((COMP, WRITERS * CAP, LANES), jnp.float32),
        cost_estimate=pl.CostEstimate(
            flops=200_000_000, bytes_accessed=11_000_000, transcendentals=0
        ),
        name=f"unpack{rows}",
    )(words, scale, recv)


def exchange(buffer, rows):
    span = span_of(rows)
    got = lax.all_to_all(buffer.reshape(WRITERS, span, LANES), G, 0, 0, tiled=True)
    return got


def local(velocity, lengths, destinations):
    vel2 = velocity.reshape(COMP * CX * CY, LANES)
    targets = destinations.reshape(NBLK // LANES, LANES)
    lens = lengths.reshape(NBLK // LANES, LANES)

    xlo, xhi, ylo, yhi, zt = faces(vel2)

    def ring(axis, n, d):
        return functools.partial(
            lax.ppermute, axis_name=axis, perm=[(i, (i + d) % n) for i in range(n)]
        )

    n_x, n_y, n_z = (lax.axis_size(a) for a in ("gx", "gy", "wa"))
    xprev, xnext = ring("gx", n_x, 1)(xhi), ring("gx", n_x, -1)(xlo)
    yprev, ynext = ring("gy", n_y, 1)(yhi), ring("gy", n_y, -1)(ylo)
    zprev, znext = ring("wa", n_z, 1)(zt), ring("wa", n_z, -1)(zt)
    words, wide, head = index(targets, lens)

    coeffs, sq = transform(vel2, xprev, xnext, yprev, ynext, zprev, znext)

    lane = lax.broadcasted_iota(jnp.int32, (1, LANES), 1)
    mine = jnp.where(lane == CAP, 0.25 * jnp.sum(sq), jnp.where(lane == CAP + 1, head[0:1], 0.0))
    for b in (1, 2):
        other = lax.ppermute(mine, "wa", [(i, i ^ b) for i in range(n_z)])
        mine = jnp.where(lane == CAP, mine + other, jnp.maximum(mine, other))
    packed = pack(words, coeffs, ROWS).reshape(WRITERS, span_of(ROWS), LANES)
    full_head = jnp.where(lane < CAP, head, mine)[:, None, :]
    packed = lax.dynamic_update_slice(packed, full_head, (0, COMP * ROWS, 0))

    got = exchange(packed, ROWS)
    inner, scale, spill = decode(got[:, COMP * ROWS, :])

    def usual(_):
        return unpack(inner, scale, got.reshape(-1, LANES), ROWS)

    def wider(_):
        again = exchange(pack(wide, coeffs, CAP), CAP)
        return unpack(inner, scale, again.reshape(-1, LANES), CAP)

    out = lax.cond(spill[0, 0] > 0, wider, usual, None)
    return out.reshape(1, 1, COMP, WRITERS, CAP, LANES)


def solution(mesh):
    return jax.shard_map(
        local,
        mesh=mesh,
        in_specs=(
            P(None, "gx", "gy", "wa"),
            P("gx", "gy", "wa", None),
            P("gx", "gy", "wa", None, None),
        ),
        out_specs=P(G, "wa", None, None, None, None),
        check_vma=False,
    )
```

```python
import functools

import jax
import jax.numpy as jnp
import numpy as np
from jax import lax
from jax.experimental import pallas as pl
from jax.experimental.pallas import tpu as pltpu
from jax.sharding import PartitionSpec as P

BY = 8
BZ = 16
LANES = 128
COMP = 3
CX = 32
CY = 64
NBLK = 2048
WRITERS = 64
CAP = 64
ROWS = 45
CELLS = 256 * 512 * 512 * 3
G = ("gx", "gy")


def span_of(rows):
    return -(-(COMP * rows + 1) // 8) * 8


def room_of(rows):
    return -(-(COMP * rows + 6) // 8) * 8


def dct_np(n):
    k = np.arange(n, dtype=np.float64)[:, None]
    j = np.arange(n, dtype=np.float64)[None, :]
    t = np.sqrt(2.0 / n) * np.cos(np.pi * (j + 0.5) * k / n)
    t[0] *= np.sqrt(0.5)
    return t


def tables_np():
    k = (0.5 * np.kron(dct_np(BY), dct_np(BZ)).T).astype(np.float32)
    high = k.astype(jnp.bfloat16)
    low = (k - high.astype(np.float32)).astype(jnp.bfloat16)
    top = np.concatenate([high, low], axis=1)
    bottom = np.concatenate([high, np.zeros_like(low)], axis=1)
    turned = [np.concatenate([np.roll(part, BZ * zb, axis=0) for part in (top, bottom)]) for zb in range(8)]
    return np.concatenate(turned, axis=0)


def iota(shape, dim):
    return lax.broadcasted_iota(jnp.int32, shape, dim)


def faces_kernel(vel, xlo, xhi, ylo, yhi, zt):
    plane = CY
    comp = CX * CY
    for n, c in enumerate((1, 2)):
        xlo[n * plane : (n + 1) * plane] = vel[c * comp : c * comp + plane]
        xhi[n * plane : (n + 1) * plane] = vel[(c + 1) * comp - plane : (c + 1) * comp]
    for n, c in enumerate((0, 2)):
        ylo[n * CX : (n + 1) * CX] = vel[pl.ds(c * comp, CX, stride=plane)]
        yhi[n * CX : (n + 1) * CX] = vel[pl.ds(c * comp + plane - 1, CX, stride=plane)]
    lane = iota((CY, LANES), 1)
    t = jnp.zeros((CY, LANES), jnp.float32)
    for k in range(2 * CX):
        f = vel[k * plane : (k + 1) * plane]
        t = jnp.where((lane >> 1) == k, pltpu.roll(f, (2 * k + 1) % LANES, 1), t)
    zt[...] = t


def faces(vel2):
    f32 = jnp.float32
    return pl.pallas_call(
        faces_kernel,
        out_shape=[
            jax.ShapeDtypeStruct((2 * CY, LANES), f32),
            jax.ShapeDtypeStruct((2 * CY, LANES), f32),
            jax.ShapeDtypeStruct((2 * CX, LANES), f32),
            jax.ShapeDtypeStruct((2 * CX, LANES), f32),
            jax.ShapeDtypeStruct((CY, LANES), f32),
        ],
        cost_estimate=pl.CostEstimate(flops=4_000_000, bytes_accessed=3_500_000, transcendentals=0),
        compiler_params=pltpu.CompilerParams(vmem_limit_bytes=10 << 20),
        name="faces",
    )(vel2)


def index_kernel(tgt, length, words, wide, head):
    chunks = NBLK // LANES
    t = tgt[...]
    ln = length[...]
    row = iota((WRITERS, LANES), 0)
    before = (iota((LANES, LANES), 0) < iota((LANES, LANES), 1)).astype(jnp.bfloat16)
    ones = jnp.ones((LANES, LANES), jnp.bfloat16)
    rhs = jnp.concatenate([before, ones], axis=1)
    hits, weighted = [], []
    for r in range(chunks):
        hit = t[r : r + 1, :] == row
        hits.append(hit)
        weighted.append(jnp.where(hit, ln[r : r + 1, :], 0).astype(jnp.float32).astype(jnp.bfloat16))
    counted = [jnp.where(h, 1.0, 0.0).astype(jnp.bfloat16) for h in hits]
    nt = (((1,), (1,)), ((), ()))
    base_l = jnp.zeros((WRITERS, LANES), jnp.float32)
    base_c = jnp.zeros((WRITERS, LANES), jnp.float32)
    lens = jnp.zeros((WRITERS, LANES), jnp.float32)
    starts = []
    for r in range(chunks):
        sums_l = jnp.dot(weighted[r], rhs, preferred_element_type=jnp.float32)
        sums_c = jnp.dot(counted[r], rhs, preferred_element_type=jnp.float32)
        start = jnp.where(hits[r], sums_l[:, :LANES] + base_l, 0.0)
        rank = jnp.where(hits[r], sums_c[:, :LANES] + base_c, 0.0)
        starts.append(jnp.sum(start, axis=0, keepdims=True))
        slot = jnp.sum(rank, axis=0, keepdims=True).astype(jnp.int32)
        at = jnp.where(slot == iota((LANES, LANES), 0), 1.0, 0.0).astype(jnp.bfloat16)
        lens += lax.dot_general(weighted[r], at, nt, preferred_element_type=jnp.float32)
        base_l += sums_l[:, LANES:]
        base_c += sums_c[:, LANES:]
    start = jnp.concatenate(starts, axis=0).astype(jnp.int32)
    first = start >> 7
    shift = start & (LANES - 1)
    words[...] = (t * room_of(ROWS) + COMP * jnp.minimum(first, ROWS)) * LANES + shift
    wide[...] = (t * room_of(CAP) + COMP * jnp.minimum(first, CAP)) * LANES + shift
    full = jnp.max(base_l, axis=0, keepdims=True)
    spill = jnp.where(full > ROWS * LANES, 1.0, 0.0)
    lane = iota((WRITERS, LANES), 1)
    head[...] = jnp.where(lane < CAP, lens, jnp.where(lane == CAP + 1, spill, 0.0))


def index(targets, lens):
    i32 = jnp.int32
    return pl.pallas_call(
        index_kernel,
        out_shape=[
            jax.ShapeDtypeStruct((NBLK // LANES, LANES), i32),
            jax.ShapeDtypeStruct((NBLK // LANES, LANES), i32),
            jax.ShapeDtypeStruct((WRITERS, LANES), jnp.float32),
        ],
        cost_estimate=pl.CostEstimate(flops=20_000_000, bytes_accessed=100_000, transcendentals=0),
        compiler_params=pltpu.CompilerParams(vmem_limit_bytes=8 << 20),
        name="index",
    )(targets, lens)


PLANES = 4
PAIR = 2


def curl_kernel(vel, xprev, xnext, yprev, ynext, zprev, znext, head, curls, mine, ends):
    comp = CX * CY
    lane = iota((CY, LANES), 1)
    row = iota((CY, LANES), 0)
    ends[...] = jnp.where(
        (lane & 1) == 0, pltpu.roll(znext[...], LANES - 1, 1), pltpu.roll(zprev[...], 1, 1)
    )
    first, last = lane == 0, lane == LANES - 1

    def plane_of(c, x):
        return vel[pl.ds(pl.multiple_of(c * comp + x * CY, CY), CY)]

    def along_x(c, x, n):
        low = jnp.maximum(x - 1, 0)
        high = jnp.minimum(x + 1, CX - 1)
        below = jnp.where(x == 0, xprev[n * CY : (n + 1) * CY], plane_of(c, low))
        above = jnp.where(x == CX - 1, xnext[n * CY : (n + 1) * CY], plane_of(c, high))
        return above - below

    def along_y(f, x, n):
        above = jnp.where(row == CY - 1, ynext[pl.ds(n * CX + x, CY, stride=0)], pltpu.roll(f, CY - 1, 0))
        below = jnp.where(row == 0, yprev[pl.ds(n * CX + x, CY, stride=0)], pltpu.roll(f, 1, 0))
        return above - below

    def along_z(f, c, x):
        edge = pltpu.roll(ends[...], LANES - 1 - 2 * (c * CX + x), 1)
        above = jnp.where(last, edge, pltpu.roll(f, LANES - 1, 1))
        below = jnp.where(first, edge, pltpu.roll(f, 1, 1))
        return above - below

    def differences(step, total):
        for p in range(PAIR):
            x = step * PAIR + p
            u, v, w = plane_of(0, x), plane_of(1, x), plane_of(2, x)
            curl = (
                along_y(w, x, 1) - along_z(v, 1, x),
                along_z(u, 0, x) - along_x(2, x, 1),
                along_x(1, x, 0) - along_y(u, x, 0),
            )
            for c in range(COMP):
                f = curl[c]
                square = f * f
                for i in range(CY // 8):
                    total += square[i * 8 : (i + 1) * 8]
                curls[pl.ds(pl.multiple_of((x * COMP + c) * CY, CY), CY)] = f
        return total

    total = lax.fori_loop(0, CX // PAIR, differences, jnp.zeros((8, LANES), jnp.float32))
    every = 0.25 * jnp.sum(total, keepdims=True)
    small = iota((8, LANES), 1)
    mine[...] = jnp.where(small == CAP, every, jnp.where(small == CAP + 1, head[0:8, :], 0.0))


def curl_of(vel2, xprev, xnext, yprev, ynext, zprev, znext, head):
    rows = COMP * NBLK
    return pl.pallas_call(
        curl_kernel,
        out_shape=[
            jax.ShapeDtypeStruct((rows, LANES), jnp.float32),
            jax.ShapeDtypeStruct((8, LANES), jnp.float32),
        ],
        scratch_shapes=[pltpu.VMEM((CY, LANES), jnp.float32)],
        cost_estimate=pl.CostEstimate(
            flops=40_000_000, bytes_accessed=7_500_000, transcendentals=0
        ),
        compiler_params=pltpu.CompilerParams(vmem_limit_bytes=16 << 20),
        name="curl",
    )(vel2, xprev, xnext, yprev, ynext, zprev, znext, head)


def transform_kernel(curls, tables, out, tiled):
    granule = iota((8, LANES), 1) >> 4
    count = PLANES * COMP

    def transform(step, carry):
        base = step * (count * CY)
        for n in range(count):
            tiles = []
            for y in range(8):
                f = curls[pl.ds(base + n * CY + (-y) % 8, 8, stride=8)]
                tiles.append(pltpu.roll(f, 16 * ((-y) % 8), 1) if y else f)
            for b in (1, 2, 4):
                moved = (granule & b) != 0
                tiles = [jnp.where(moved, tiles[(j - b) % 8], tiles[j]) for j in range(8)]
            for zb in range(8):
                tiled[zb * count * 8 + n * 8 : zb * count * 8 + n * 8 + 8] = tiles[zb]
        for zb in range(8):
            whole = tiled[zb * count * 8 : (zb + 1) * count * 8]
            high = whole.astype(jnp.bfloat16)
            low = (whole - high.astype(jnp.float32)).astype(jnp.bfloat16)
            both = jnp.dot(
                jnp.concatenate([high, low], axis=1),
                tables[zb * 256 : zb * 256 + 256],
                preferred_element_type=jnp.float32,
            )
            coeffs = both[:, :LANES] + both[:, LANES:]
            for n in range(count):
                p, c = n // COMP, n % COMP
                at = base + COMP * (p * CY + zb * 8) + c
                out[pl.ds(at, 8, stride=COMP)] = coeffs[n * 8 : n * 8 + 8]
        return carry

    lax.fori_loop(0, CX // PLANES, transform, 0)


def transform_of(curls):
    tables = jnp.asarray(tables_np())
    rows = COMP * NBLK
    return pl.pallas_call(
        transform_kernel,
        out_shape=jax.ShapeDtypeStruct((rows, LANES), jnp.float32),
        scratch_shapes=[pltpu.VMEM((PLANES * COMP * CY, LANES), jnp.float32)],
        cost_estimate=pl.CostEstimate(
            flops=2 * rows * 256 * 256, bytes_accessed=7_500_000, transcendentals=0
        ),
        compiler_params=pltpu.CompilerParams(vmem_limit_bytes=16 << 20),
        name="transform",
    )(curls, tables)


def pack_kernel(rows, words, coeffs, head, one, two, three, four, out, room):
    lane = iota((COMP, LANES), 1)
    span, local_span = span_of(rows), room_of(rows)

    def body(r, carry):
        for j in range(LANES):
            p, yb, zb = j // CY, (j % CY) // 8, j % 8
            word = words[r, j]
            addr = word >> 7
            value = coeffs[pl.ds(r * (COMP * LANES) + COMP * (p * CY + zb * 8 + yb), COMP)]
            value = pltpu.roll(value, word, 1)
            kept = lane >= (jnp.full((COMP, LANES), word, jnp.int32) & (LANES - 1))
            pltpu.store(room.at[pl.ds(addr, COMP)], value, mask=kept)
            room[pl.ds(addr + COMP, COMP)] = value
        return carry

    lax.fori_loop(0, NBLK // LANES, body, 0)

    def settle(w, carry):
        source = pl.multiple_of(w * local_span, 8)
        target = pl.multiple_of(w * span, 8)
        out[pl.ds(target, span)] = room[pl.ds(source, span)]
        return carry

    lax.fori_loop(0, WRITERS, settle, 0)
    small = iota((8, LANES), 1)
    both = jnp.where(
        small == CAP,
        (one[...] + two[...]) + (three[...] + four[...]),
        jnp.maximum(jnp.maximum(one[...], two[...]), jnp.maximum(three[...], four[...])),
    )
    for w in range(0, WRITERS, 8):
        out[pl.ds(w * span + COMP * rows, 8, stride=span)] = jnp.where(
            small < CAP, head[w : w + 8], both
        )


def pack(words, coeffs, head, sums, rows):
    span = span_of(rows)
    return pl.pallas_call(
        functools.partial(pack_kernel, rows),
        in_specs=[
            pl.BlockSpec(memory_space=pltpu.SMEM),
            *[pl.BlockSpec(memory_space=pltpu.VMEM)] * 6,
        ],
        out_specs=pl.BlockSpec(memory_space=pltpu.VMEM),
        out_shape=jax.ShapeDtypeStruct((WRITERS * span, LANES), jnp.float32),
        scratch_shapes=[pltpu.VMEM((WRITERS * room_of(rows), LANES), jnp.float32)],
        cost_estimate=pl.CostEstimate(
            flops=200_000_000, bytes_accessed=8_000_000, transcendentals=0
        ),
        compiler_params=pltpu.CompilerParams(vmem_limit_bytes=22 << 20),
        name=f"pack{rows}",
    )(words, coeffs, head, *sums)


SOURCES = 8
ABREAST = 4


def unpack_kernel(rows, head, recv, out, spill, at_s, cut_s, at_v, cut_v, scale, sem):
    step = pl.program_id(0)
    span = span_of(rows)

    @pl.when(step == 0)
    def _():
        h = head[...].reshape(WRITERS, LANES) if head.shape[1] == 1 else head[:, 7, :]
        lane = iota((WRITERS, LANES), 1)
        lens = jnp.where(lane < CAP, h, 0.0)
        before = (iota((LANES, LANES), 0) < iota((LANES, LANES), 1)).astype(jnp.bfloat16)
        start = jnp.dot(lens.astype(jnp.bfloat16), before, preferred_element_type=jnp.float32)
        start = start.astype(jnp.int32)
        first = start >> 7
        turn = start & (LANES - 1)
        at = iota((WRITERS, LANES), 0) * span + COMP * jnp.minimum(first, rows - 2)
        at_v[...] = at * LANES + ((LANES - turn) & (LANES - 1))
        split = jnp.where(first >= rows - 1, LANES, turn)
        cut_v[...] = lens.astype(jnp.int32) + 256 * split
        copies = [
            pltpu.make_async_copy(v, s, sem.at[i])
            for i, (v, s) in enumerate(((at_v, at_s), (cut_v, cut_s)))
        ]
        for copy in copies:
            copy.start()
        total = jnp.sum(jnp.where(lane == CAP, h, 0.0), keepdims=True)
        rms = jnp.sqrt(total * (1.0 / CELLS) + 1e-6)
        scale[...] = jnp.broadcast_to(1.0 / rms, scale.shape)
        flag = jnp.max(jnp.where(lane == CAP + 1, h, 0.0), keepdims=True)
        spill[...] = jnp.broadcast_to(flag, spill.shape).astype(jnp.int32)
        for copy in copies:
            copy.wait()

    factor = scale[0:COMP]
    lane = iota((COMP, LANES), 1)
    flat = out.reshape(COMP * SOURCES * CAP, LANES)

    def body(s, carry):
        for k in range(ABREAST * CAP):
            number, q = step * SOURCES + s * ABREAST + k // CAP, k % CAP
            word = at_s[number, q]
            cut = jnp.full((COMP, LANES), cut_s[number, q], jnp.int32)
            at = word >> 7
            one = recv[pl.ds(at, COMP)]
            two = recv[pl.ds(at + COMP, COMP)]
            value = jnp.where(lane >= (cut >> 8), one, two)
            value = pltpu.roll(value, word, 1)
            value = jnp.where(lane < (cut & 255), value * factor, 0.0)
            flat[pl.ds(s * (ABREAST * CAP) + k, COMP, stride=SOURCES * CAP)] = value
        return carry

    lax.fori_loop(0, SOURCES // ABREAST, body, 0)


def unpack(head, recv, rows):
    if head.shape[1] == 1:
        head_spec = pl.BlockSpec(head.shape, lambda i: (0, 0, 0))
    else:
        head_spec = pl.BlockSpec((WRITERS, 8, LANES), lambda i: (0, head.shape[1] // 8 - 1, 0))
    return pl.pallas_call(
        functools.partial(unpack_kernel, rows),
        grid=(WRITERS // SOURCES,),
        in_specs=[head_spec, pl.BlockSpec(recv.shape, lambda i: (0, 0))],
        out_specs=[
            pl.BlockSpec((COMP, SOURCES * CAP, LANES), lambda i: (0, i, 0)),
            pl.BlockSpec((8, LANES), lambda i: (0, 0)),
        ],
        out_shape=[
            jax.ShapeDtypeStruct((COMP, WRITERS * CAP, LANES), jnp.float32),
            jax.ShapeDtypeStruct((8, LANES), jnp.int32),
        ],
        scratch_shapes=[
            *[pltpu.SMEM((WRITERS, LANES), jnp.int32)] * 2,
            *[pltpu.VMEM((WRITERS, LANES), jnp.int32)] * 2,
            pltpu.VMEM((8, LANES), jnp.float32),
            pltpu.SemaphoreType.DMA((2,)),
        ],
        cost_estimate=pl.CostEstimate(
            flops=200_000_000, bytes_accessed=11_000_000, transcendentals=0
        ),
        compiler_params=pltpu.CompilerParams(vmem_limit_bytes=24 << 20),
        name=f"unpack{rows}",
    )(head, recv)


def exchange(buffer, rows):
    return lax.all_to_all(
        buffer.reshape(WRITERS, span_of(rows), LANES), G, 0, 0, tiled=True
    )


def local(velocity, lengths, destinations):
    vel2 = velocity.reshape(COMP * CX * CY, LANES)
    targets = destinations.reshape(NBLK // LANES, LANES)
    lens = lengths.reshape(NBLK // LANES, LANES)

    xlo, xhi, ylo, yhi, zt = faces(vel2)

    def ring(axis, n, d):
        return functools.partial(
            lax.ppermute, axis_name=axis, perm=[(i, (i + d) % n) for i in range(n)]
        )

    n_x, n_y, n_z = (lax.axis_size(a) for a in ("gx", "gy", "wa"))
    xprev, xnext = ring("gx", n_x, 1)(xhi), ring("gx", n_x, -1)(xlo)
    yprev, ynext = ring("gy", n_y, 1)(yhi), ring("gy", n_y, -1)(ylo)
    zprev, znext = ring("wa", n_z, 1)(zt), ring("wa", n_z, -1)(zt)
    words, wide, head = index(targets, lens)

    curls, mine = curl_of(vel2, xprev, xnext, yprev, ynext, zprev, znext, head)
    sums = [mine] + [ring("wa", n_z, d)(mine) for d in range(1, n_z)]
    coeffs = transform_of(curls)
    packed = pack(words, coeffs, head, sums, ROWS)
    got = exchange(packed, ROWS)
    out, spill = unpack(got, got.reshape(-1, LANES), ROWS)

    def again(carry):
        more = exchange(pack(wide, coeffs, head, sums, CAP), CAP)
        wider, _ = unpack(got[:, COMP * ROWS :, :], more.reshape(-1, LANES), CAP)
        return jnp.int32(0), wider

    _, out = lax.while_loop(lambda carry: carry[0] > 0, again, (spill[0, 0], out))
    return out.reshape(1, 1, COMP, WRITERS, CAP, LANES)


def solution(mesh):
    return jax.shard_map(
        local,
        mesh=mesh,
        in_specs=(
            P(None, "gx", "gy", "wa"),
            P("gx", "gy", "wa", None),
            P("gx", "gy", "wa", None, None),
        ),
        out_specs=P(G, "wa", None, None, None, None),
        check_vma=False,
    )
```

```python
import functools

import jax
import jax.numpy as jnp
import numpy as np
from jax import lax
from jax.experimental import pallas as pl
from jax.experimental.pallas import tpu as pltpu
from jax.sharding import PartitionSpec as P

BY = 8
BZ = 16
LANES = 128
COMP = 3
CX = 32
CY = 64
NBLK = 2048
WRITERS = 64
CAP = 64
ROWS = 45
CELLS = 256 * 512 * 512 * 3
G = ("gx", "gy")


def span_of(rows):
    return -(-(COMP * rows + 1) // 8) * 8


def room_of(rows):
    return -(-(COMP * rows + 6) // 8) * 8


def dct_np(n):
    k = np.arange(n, dtype=np.float64)[:, None]
    j = np.arange(n, dtype=np.float64)[None, :]
    t = np.sqrt(2.0 / n) * np.cos(np.pi * (j + 0.5) * k / n)
    t[0] *= np.sqrt(0.5)
    return t


def tables_np():
    k = (0.5 * np.kron(dct_np(BY), dct_np(BZ)).T).astype(np.float32)
    high = k.astype(jnp.bfloat16)
    low = (k - high.astype(np.float32)).astype(jnp.bfloat16)
    top = np.concatenate([high, low], axis=1)
    bottom = np.concatenate([high, np.zeros_like(low)], axis=1)
    turned = [np.concatenate([np.roll(part, BZ * zb, axis=0) for part in (top, bottom)]) for zb in range(8)]
    return np.concatenate(turned, axis=0)


def iota(shape, dim):
    return lax.broadcasted_iota(jnp.int32, shape, dim)


def faces_kernel(vel, xlo, xhi, ylo, yhi, zt, held):
    plane = CY
    comp = CX * CY
    for n, c in enumerate((1, 2)):
        xlo[n * plane : (n + 1) * plane] = vel[c * comp : c * comp + plane]
        xhi[n * plane : (n + 1) * plane] = vel[(c + 1) * comp - plane : (c + 1) * comp]
    for n, c in enumerate((0, 2)):
        ylo[n * CX : (n + 1) * CX] = vel[pl.ds(c * comp, CX, stride=plane)]
        yhi[n * CX : (n + 1) * CX] = vel[pl.ds(c * comp + plane - 1, CX, stride=plane)]
    lane = iota((CY, LANES), 1)
    t = jnp.zeros((CY, LANES), jnp.float32)
    for k in range(2 * CX):
        f = vel[k * plane : (k + 1) * plane]
        t = jnp.where((lane >> 1) == k, pltpu.roll(f, (2 * k + 1) % LANES, 1), t)
    zt[...] = t
    held[...] = vel[...]


def faces(vel2):
    f32 = jnp.float32
    return pl.pallas_call(
        faces_kernel,
        out_shape=[
            jax.ShapeDtypeStruct((2 * CY, LANES), f32),
            jax.ShapeDtypeStruct((2 * CY, LANES), f32),
            jax.ShapeDtypeStruct((2 * CX, LANES), f32),
            jax.ShapeDtypeStruct((2 * CX, LANES), f32),
            jax.ShapeDtypeStruct((CY, LANES), f32),
            jax.ShapeDtypeStruct(vel2.shape, f32),
        ],
        cost_estimate=pl.CostEstimate(flops=4_000_000, bytes_accessed=3_500_000, transcendentals=0),
        compiler_params=pltpu.CompilerParams(vmem_limit_bytes=10 << 20),
        name="faces",
    )(vel2)


def index_kernel(mixed, words, wide, head):
    chunks = NBLK // LANES
    t = mixed[...] >> 8
    ln = mixed[...] & 255
    row = iota((WRITERS, LANES), 0)
    before = (iota((LANES, LANES), 0) < iota((LANES, LANES), 1)).astype(jnp.bfloat16)
    ones = jnp.ones((LANES, LANES), jnp.bfloat16)
    rhs = jnp.concatenate([before, ones], axis=1)
    hits, weighted = [], []
    for r in range(chunks):
        hit = t[r : r + 1, :] == row
        hits.append(hit)
        weighted.append(jnp.where(hit, ln[r : r + 1, :], 0).astype(jnp.float32).astype(jnp.bfloat16))
    counted = [jnp.where(h, 1.0, 0.0).astype(jnp.bfloat16) for h in hits]
    nt = (((1,), (1,)), ((), ()))
    base_l = jnp.zeros((WRITERS, LANES), jnp.float32)
    base_c = jnp.zeros((WRITERS, LANES), jnp.float32)
    lens = jnp.zeros((WRITERS, LANES), jnp.float32)
    starts = []
    for r in range(chunks):
        sums_l = jnp.dot(weighted[r], rhs, preferred_element_type=jnp.float32)
        sums_c = jnp.dot(counted[r], rhs, preferred_element_type=jnp.float32)
        start = jnp.where(hits[r], sums_l[:, :LANES] + base_l, 0.0)
        rank = jnp.where(hits[r], sums_c[:, :LANES] + base_c, 0.0)
        starts.append(jnp.sum(start, axis=0, keepdims=True))
        slot = jnp.sum(rank, axis=0, keepdims=True).astype(jnp.int32)
        at = jnp.where(slot == iota((LANES, LANES), 0), 1.0, 0.0).astype(jnp.bfloat16)
        lens += lax.dot_general(weighted[r], at, nt, preferred_element_type=jnp.float32)
        base_l += sums_l[:, LANES:]
        base_c += sums_c[:, LANES:]
    start = jnp.concatenate(starts, axis=0).astype(jnp.int32)
    first = start >> 7
    shift = start & (LANES - 1)
    words[...] = (t * room_of(ROWS) + COMP * jnp.minimum(first, ROWS)) * LANES + shift
    wide[...] = (t * room_of(CAP) + COMP * jnp.minimum(first, CAP)) * LANES + shift
    full = jnp.max(base_l, axis=0, keepdims=True)
    spill = jnp.where(full > ROWS * LANES, 1.0, 0.0)
    lane = iota((WRITERS, LANES), 1)
    head[...] = jnp.where(lane < CAP, lens, jnp.where(lane == CAP + 1, spill, 0.0))


def index(mixed):
    i32 = jnp.int32
    return pl.pallas_call(
        index_kernel,
        out_shape=[
            jax.ShapeDtypeStruct((NBLK // LANES, LANES), i32),
            jax.ShapeDtypeStruct((NBLK // LANES, LANES), i32),
            jax.ShapeDtypeStruct((WRITERS, LANES), jnp.float32),
        ],
        cost_estimate=pl.CostEstimate(flops=20_000_000, bytes_accessed=100_000, transcendentals=0),
        compiler_params=pltpu.CompilerParams(vmem_limit_bytes=8 << 20),
        name="index",
    )(mixed)


PLANES = 4
PAIR = 2


def curl_kernel(vel, xprev, xnext, yprev, ynext, zprev, znext, head, curls, mine, ends):
    comp = CX * CY
    lane = iota((CY, LANES), 1)
    row = iota((CY, LANES), 0)
    ends[...] = jnp.where(
        (lane & 1) == 0, pltpu.roll(znext[...], LANES - 1, 1), pltpu.roll(zprev[...], 1, 1)
    )
    first, last = lane == 0, lane == LANES - 1

    def plane_of(c, x):
        return vel[pl.ds(pl.multiple_of(c * comp + x * CY, CY), CY)]

    def along_x(c, x, n):
        low = jnp.maximum(x - 1, 0)
        high = jnp.minimum(x + 1, CX - 1)
        below = jnp.where(x == 0, xprev[n * CY : (n + 1) * CY], plane_of(c, low))
        above = jnp.where(x == CX - 1, xnext[n * CY : (n + 1) * CY], plane_of(c, high))
        return above - below

    def along_y(f, x, n):
        above = jnp.where(row == CY - 1, ynext[pl.ds(n * CX + x, CY, stride=0)], pltpu.roll(f, CY - 1, 0))
        below = jnp.where(row == 0, yprev[pl.ds(n * CX + x, CY, stride=0)], pltpu.roll(f, 1, 0))
        return above - below

    def along_z(f, c, x):
        edge = pltpu.roll(ends[...], LANES - 1 - 2 * (c * CX + x), 1)
        above = jnp.where(last, edge, pltpu.roll(f, LANES - 1, 1))
        below = jnp.where(first, edge, pltpu.roll(f, 1, 1))
        return above - below

    def differences(step, total):
        for p in range(PAIR):
            x = step * PAIR + p
            u, v, w = plane_of(0, x), plane_of(1, x), plane_of(2, x)
            curl = (
                along_y(w, x, 1) - along_z(v, 1, x),
                along_z(u, 0, x) - along_x(2, x, 1),
                along_x(1, x, 0) - along_y(u, x, 0),
            )
            for c in range(COMP):
                f = curl[c]
                square = f * f
                for i in range(CY // 8):
                    total += square[i * 8 : (i + 1) * 8]
                curls[pl.ds(pl.multiple_of((x * COMP + c) * CY, CY), CY)] = f
        return total

    total = lax.fori_loop(0, CX // PAIR, differences, jnp.zeros((8, LANES), jnp.float32))
    every = 0.25 * jnp.sum(total, keepdims=True)
    small = iota((8, LANES), 1)
    mine[...] = jnp.where(small == CAP, every, jnp.where(small == CAP + 1, head[0:8, :], 0.0))


def curl_of(vel2, xprev, xnext, yprev, ynext, zprev, znext, head):
    rows = COMP * NBLK
    return pl.pallas_call(
        curl_kernel,
        out_shape=[
            jax.ShapeDtypeStruct((rows, LANES), jnp.float32),
            jax.ShapeDtypeStruct((8, LANES), jnp.float32),
        ],
        scratch_shapes=[pltpu.VMEM((CY, LANES), jnp.float32)],
        cost_estimate=pl.CostEstimate(
            flops=40_000_000, bytes_accessed=7_500_000, transcendentals=0
        ),
        compiler_params=pltpu.CompilerParams(vmem_limit_bytes=16 << 20),
        name="curl",
    )(vel2, xprev, xnext, yprev, ynext, zprev, znext, head)


def transform_kernel(curls, tables, out, tiled):
    granule = iota((8, LANES), 1) >> 4
    count = PLANES * COMP

    def transform(step, carry):
        base = step * (count * CY)
        for n in range(count):
            tiles = []
            for y in range(8):
                f = curls[pl.ds(base + n * CY + (-y) % 8, 8, stride=8)]
                tiles.append(pltpu.roll(f, 16 * ((-y) % 8), 1) if y else f)
            for b in (1, 2, 4):
                moved = (granule & b) != 0
                tiles = [jnp.where(moved, tiles[(j - b) % 8], tiles[j]) for j in range(8)]
            for zb in range(8):
                tiled[zb * count * 8 + n * 8 : zb * count * 8 + n * 8 + 8] = tiles[zb]
        for zb in range(8):
            whole = tiled[zb * count * 8 : (zb + 1) * count * 8]
            high = whole.astype(jnp.bfloat16)
            low = (whole - high.astype(jnp.float32)).astype(jnp.bfloat16)
            both = jnp.dot(
                jnp.concatenate([high, low], axis=1),
                tables[zb * 256 : zb * 256 + 256],
                preferred_element_type=jnp.float32,
            )
            coeffs = both[:, :LANES] + both[:, LANES:]
            for n in range(count):
                p, c = n // COMP, n % COMP
                at = base + COMP * (p * CY + zb * 8) + c
                out[pl.ds(at, 8, stride=COMP)] = coeffs[n * 8 : n * 8 + 8]
        return carry

    lax.fori_loop(0, CX // PLANES, transform, 0)


def transform_of(curls):
    tables = jnp.asarray(tables_np())
    rows = COMP * NBLK
    return pl.pallas_call(
        transform_kernel,
        out_shape=jax.ShapeDtypeStruct((rows, LANES), jnp.float32),
        scratch_shapes=[pltpu.VMEM((PLANES * COMP * CY, LANES), jnp.float32)],
        cost_estimate=pl.CostEstimate(
            flops=2 * rows * 256 * 256, bytes_accessed=7_500_000, transcendentals=0
        ),
        compiler_params=pltpu.CompilerParams(vmem_limit_bytes=16 << 20),
        name="transform",
    )(curls, tables)


WIDTH = 2


def pack_kernel(rows, words, coeffs, head, one, two, three, four, out, room):
    lane = iota((COMP, LANES), 1)
    span, local_span = span_of(rows), room_of(rows)

    def body(r, carry):
        for j in range(WIDTH * LANES):
            p, yb, zb = j // CY, (j % CY) // 8, j % 8
            word = words[r * WIDTH + j // LANES, j % LANES]
            addr = word >> 7
            source = COMP * (p * CY + zb * 8 + yb)
            value = coeffs[pl.ds(r * (COMP * WIDTH * LANES) + source, COMP)]
            value = pltpu.roll(value, word, 1)
            kept = lane >= (jnp.full((COMP, LANES), word, jnp.int32) & (LANES - 1))
            pltpu.store(room.at[pl.ds(addr, COMP)], value, mask=kept)
            room[pl.ds(addr + COMP, COMP)] = value
        return carry

    lax.fori_loop(0, NBLK // LANES // WIDTH, body, 0)

    def settle(w, carry):
        source = pl.multiple_of(w * local_span, 8)
        target = pl.multiple_of(w * span, 8)
        out[pl.ds(target, span)] = room[pl.ds(source, span)]
        return carry

    lax.fori_loop(0, WRITERS, settle, 0)
    small = iota((8, LANES), 1)
    both = jnp.where(
        small == CAP,
        (one[...] + two[...]) + (three[...] + four[...]),
        jnp.maximum(jnp.maximum(one[...], two[...]), jnp.maximum(three[...], four[...])),
    )
    for w in range(0, WRITERS, 8):
        out[pl.ds(w * span + COMP * rows, 8, stride=span)] = jnp.where(
            small < CAP, head[w : w + 8], both
        )


def pack(words, coeffs, head, sums, rows):
    span = span_of(rows)
    return pl.pallas_call(
        functools.partial(pack_kernel, rows),
        in_specs=[
            pl.BlockSpec(memory_space=pltpu.SMEM),
            *[pl.BlockSpec(memory_space=pltpu.VMEM)] * 6,
        ],
        out_specs=pl.BlockSpec(memory_space=pltpu.VMEM),
        out_shape=jax.ShapeDtypeStruct((WRITERS * span, LANES), jnp.float32),
        scratch_shapes=[pltpu.VMEM((WRITERS * room_of(rows), LANES), jnp.float32)],
        cost_estimate=pl.CostEstimate(
            flops=200_000_000, bytes_accessed=8_000_000, transcendentals=0
        ),
        compiler_params=pltpu.CompilerParams(vmem_limit_bytes=22 << 20),
        name=f"pack{rows}",
    )(words, coeffs, head, *sums)


SOURCES = 8
ABREAST = 8


def unpack_kernel(rows, *refs):
    head = None
    if len(refs) == 10:
        head, refs = refs[0], refs[1:]
    recv, out, spill, heads, words_s, words_v, scale, pieces, sem = refs
    step = pl.program_id(0)
    span = span_of(rows)

    @pl.when(step == 0)
    def _():
        if head is None:
            h = recv[pl.ds(COMP * rows, WRITERS, stride=span)]
        else:
            h = head[...]
        heads[...] = h
        lane = iota((WRITERS, LANES), 1)
        lens = jnp.where(lane < CAP, h, 0.0)
        before = (iota((LANES, LANES), 0) < iota((LANES, LANES), 1)).astype(jnp.bfloat16)
        start = jnp.dot(lens.astype(jnp.bfloat16), before, preferred_element_type=jnp.float32)
        start = start.astype(jnp.int32)
        first = start >> 7
        turn = start & (LANES - 1)
        at = iota((WRITERS, LANES), 0) * span + COMP * jnp.minimum(first, rows - 2)
        late = (first >= rows - 1).astype(jnp.int32)
        words_v[...] = (
            (at << 17) + (lens.astype(jnp.int32) << 9) + (late << 8) + (LANES - turn)
        )
        copy = pltpu.make_async_copy(words_v, words_s, sem)
        copy.start()
        total = jnp.sum(jnp.where(lane == CAP, h, 0.0), keepdims=True)
        rms = jnp.sqrt(total * (1.0 / CELLS) + 1e-6)
        scale[...] = jnp.broadcast_to(1.0 / rms, scale.shape)
        spill[0, 0] = jnp.max(jnp.where(lane == CAP + 1, h, 0.0)).astype(jnp.int32)
        copy.wait()

    factor = scale[...]
    lane = iota((COMP, LANES), 1)

    def body(s, carry):
        for k in range(ABREAST * CAP):
            number, q = step * SOURCES + s * ABREAST + k // CAP, k % CAP
            word = words_s[number, q]
            marks = jnp.full((COMP, LANES), word, jnp.int32)
            at = word >> 17
            one = recv[pl.ds(at, COMP)]
            two = recv[pl.ds(at + COMP, COMP)]
            inside = ((marks & 511) + lane) & 384
            value = jnp.where(inside == LANES, one, two)
            value = pltpu.roll(value, word, 1)
            value = jnp.where(lane < ((marks >> 9) & 255), value, 0.0)
            pieces[k * 4 : k * 4 + COMP] = value
        for k in range(0, ABREAST * CAP, 8):
            for c in range(COMP):
                row = pl.multiple_of(s * (ABREAST * CAP) + k, 8)
                out[c, pl.ds(row, 8)] = pieces[pl.ds(k * 4 + c, 8, stride=4)] * factor
        return carry

    lax.fori_loop(0, SOURCES // ABREAST, body, 0)


def unpack(recv, rows, head=None):
    args = (recv,) if head is None else (head, recv)
    return pl.pallas_call(
        functools.partial(unpack_kernel, rows),
        grid=(WRITERS // SOURCES,),
        in_specs=[pl.BlockSpec(a.shape, lambda i: (0, 0)) for a in args],
        out_specs=[
            pl.BlockSpec((COMP, SOURCES * CAP, LANES), lambda i: (0, i, 0)),
            pl.BlockSpec(memory_space=pltpu.SMEM),
            pl.BlockSpec((WRITERS, LANES), lambda i: (0, 0)),
        ],
        out_shape=[
            jax.ShapeDtypeStruct((COMP, WRITERS * CAP, LANES), jnp.float32),
            jax.ShapeDtypeStruct((1, 1), jnp.int32),
            jax.ShapeDtypeStruct((WRITERS, LANES), jnp.float32),
        ],
        scratch_shapes=[
            pltpu.SMEM((WRITERS, LANES), jnp.int32),
            pltpu.VMEM((WRITERS, LANES), jnp.int32),
            pltpu.VMEM((8, LANES), jnp.float32),
            pltpu.VMEM((ABREAST * CAP * 4, LANES), jnp.float32),
            pltpu.SemaphoreType.DMA,
        ],
        cost_estimate=pl.CostEstimate(
            flops=200_000_000, bytes_accessed=11_000_000, transcendentals=0
        ),
        compiler_params=pltpu.CompilerParams(vmem_limit_bytes=24 << 20),
        name=f"unpack{rows}",
    )(*args)


def exchange(buffer, rows):
    return lax.all_to_all(
        buffer.reshape(WRITERS, span_of(rows), LANES), G, 0, 0, tiled=True
    )


def local(velocity, lengths, destinations):
    vel2 = velocity.reshape(COMP * CX * CY, LANES)
    targets = destinations.reshape(NBLK // LANES, LANES)
    lens = lengths.reshape(NBLK // LANES, LANES)

    xlo, xhi, ylo, yhi, zt, vel2 = faces(vel2)

    def ring(axis, n, d):
        return functools.partial(
            lax.ppermute, axis_name=axis, perm=[(i, (i + d) % n) for i in range(n)]
        )

    n_x, n_y, n_z = (lax.axis_size(a) for a in ("gx", "gy", "wa"))
    xprev, xnext = ring("gx", n_x, 1)(xhi), ring("gx", n_x, -1)(xlo)
    yprev, ynext = ring("gy", n_y, 1)(yhi), ring("gy", n_y, -1)(ylo)
    zprev, znext = ring("wa", n_z, 1)(zt), ring("wa", n_z, -1)(zt)
    words, wide, head = index(targets * 256 + lens)

    curls, mine = curl_of(vel2, xprev, xnext, yprev, ynext, zprev, znext, head)
    sums = [mine] + [ring("wa", n_z, d)(mine) for d in range(1, n_z)]
    coeffs = transform_of(curls)
    packed = pack(words, coeffs, head, sums, ROWS)
    got = exchange(packed, ROWS)
    out, spill, heads = unpack(got.reshape(-1, LANES), ROWS)

    def again(carry):
        more = exchange(pack(wide, coeffs, head, sums, CAP), CAP)
        wider, _, _ = unpack(more.reshape(-1, LANES), CAP, heads)
        return jnp.int32(0), wider

    _, out = lax.while_loop(lambda carry: carry[0] > 0, again, (spill.reshape(()), out))
    return out.reshape(1, 1, COMP, WRITERS, CAP, LANES)


def solution(mesh):
    return jax.shard_map(
        local,
        mesh=mesh,
        in_specs=(
            P(None, "gx", "gy", "wa"),
            P("gx", "gy", "wa", None),
            P("gx", "gy", "wa", None, None),
        ),
        out_specs=P(G, "wa", None, None, None, None),
        check_vma=False,
    )
```

```python
import functools

import jax
import jax.numpy as jnp
import numpy as np
from jax import lax
from jax.experimental import pallas as pl
from jax.experimental.pallas import tpu as pltpu
from jax.sharding import PartitionSpec as P


BY = 8
BZ = 16
LANES = 128
COMP = 3
CX = 32
CY = 64
NBLK = 2048
WRITERS = 64
CAP = 64
ROWS = 45
CELLS = 256 * 512 * 512 * 3
G = ("gx", "gy")


def span_of(rows):
    return -(-(COMP * rows + 1) // 8) * 8


def room_of(rows):
    return -(-(COMP * rows + 6) // 8) * 8


def dct_np(n):
    k = np.arange(n, dtype=np.float64)[:, None]
    j = np.arange(n, dtype=np.float64)[None, :]
    t = np.sqrt(2.0 / n) * np.cos(np.pi * (j + 0.5) * k / n)
    t[0] *= np.sqrt(0.5)
    return t


def tables_np():
    k = (0.5 * np.kron(dct_np(BY), dct_np(BZ)).T).astype(np.float32)
    high = k.astype(jnp.bfloat16)
    low = (k - high.astype(np.float32)).astype(jnp.bfloat16)
    top = np.concatenate([high, low], axis=1)
    bottom = np.concatenate([high, np.zeros_like(low)], axis=1)
    turned = [np.concatenate([np.roll(part, BZ * zb, axis=0) for part in (top, bottom)]) for zb in range(8)]
    return np.concatenate(turned, axis=0)


def iota(shape, dim):
    return lax.broadcasted_iota(jnp.int32, shape, dim)


def faces_kernel(vel, xlo, xhi, ylo, yhi, zt, held):
    plane = CY
    comp = CX * CY
    for n, c in enumerate((1, 2)):
        xlo[n * plane : (n + 1) * plane] = vel[c * comp : c * comp + plane]
        xhi[n * plane : (n + 1) * plane] = vel[(c + 1) * comp - plane : (c + 1) * comp]
    for n, c in enumerate((0, 2)):
        ylo[n * CX : (n + 1) * CX] = vel[pl.ds(c * comp, CX, stride=plane)]
        yhi[n * CX : (n + 1) * CX] = vel[pl.ds(c * comp + plane - 1, CX, stride=plane)]
    lane = iota((CY, LANES), 1)
    t = jnp.zeros((CY, LANES), jnp.float32)
    for k in range(2 * CX):
        f = vel[k * plane : (k + 1) * plane]
        t = jnp.where((lane >> 1) == k, pltpu.roll(f, (2 * k + 1) % LANES, 1), t)
    zt[...] = t
    held[...] = vel[...]


def faces(vel2):
    f32 = jnp.float32
    return pl.pallas_call(
        faces_kernel,
        out_shape=[
            jax.ShapeDtypeStruct((2 * CY, LANES), f32),
            jax.ShapeDtypeStruct((2 * CY, LANES), f32),
            jax.ShapeDtypeStruct((2 * CX, LANES), f32),
            jax.ShapeDtypeStruct((2 * CX, LANES), f32),
            jax.ShapeDtypeStruct((CY, LANES), f32),
            jax.ShapeDtypeStruct(vel2.shape, f32),
        ],
        cost_estimate=pl.CostEstimate(flops=4_000_000, bytes_accessed=3_500_000, transcendentals=0),
        compiler_params=pltpu.CompilerParams(vmem_limit_bytes=10 << 20),
        name="faces",
    )(vel2)


def index_kernel(mixed, ylo_in, yhi_in, zt_in, words, wide, head, ylo, yhi, zt):
    ylo[...], yhi[...], zt[...] = ylo_in[...], yhi_in[...], zt_in[...]
    chunks = NBLK // LANES
    t = mixed[...] >> 8
    ln = mixed[...] & 255
    row = iota((WRITERS, LANES), 0)
    before = (iota((LANES, LANES), 0) < iota((LANES, LANES), 1)).astype(jnp.bfloat16)
    ones = jnp.ones((LANES, LANES), jnp.bfloat16)
    rhs = jnp.concatenate([before, ones], axis=1)
    hits, weighted = [], []
    for r in range(chunks):
        hit = t[r : r + 1, :] == row
        hits.append(hit)
        weighted.append(jnp.where(hit, ln[r : r + 1, :], 0).astype(jnp.float32).astype(jnp.bfloat16))
    counted = [jnp.where(h, 1.0, 0.0).astype(jnp.bfloat16) for h in hits]
    nt = (((1,), (1,)), ((), ()))
    base_l = jnp.zeros((WRITERS, LANES), jnp.float32)
    base_c = jnp.zeros((WRITERS, LANES), jnp.float32)
    lens = jnp.zeros((WRITERS, LANES), jnp.float32)
    starts = []
    for r in range(chunks):
        sums_l = jnp.dot(weighted[r], rhs, preferred_element_type=jnp.float32)
        sums_c = jnp.dot(counted[r], rhs, preferred_element_type=jnp.float32)
        start = jnp.where(hits[r], sums_l[:, :LANES] + base_l, 0.0)
        rank = jnp.where(hits[r], sums_c[:, :LANES] + base_c, 0.0)
        starts.append(jnp.sum(start, axis=0, keepdims=True))
        slot = jnp.sum(rank, axis=0, keepdims=True).astype(jnp.int32)
        at = jnp.where(slot == iota((LANES, LANES), 0), 1.0, 0.0).astype(jnp.bfloat16)
        lens += lax.dot_general(weighted[r], at, nt, preferred_element_type=jnp.float32)
        base_l += sums_l[:, LANES:]
        base_c += sums_c[:, LANES:]
    start = jnp.concatenate(starts, axis=0).astype(jnp.int32)
    first = start >> 7
    shift = start & (LANES - 1)
    words[...] = (t * room_of(ROWS) + COMP * jnp.minimum(first, ROWS)) * LANES + shift
    wide[...] = (t * room_of(CAP) + COMP * jnp.minimum(first, CAP)) * LANES + shift
    full = jnp.max(base_l, axis=0, keepdims=True)
    spill = jnp.where(full > ROWS * LANES, 1.0, 0.0)
    lane = iota((WRITERS, LANES), 1)
    head[...] = jnp.where(lane < CAP, lens, jnp.where(lane == CAP + 1, spill, 0.0))


def index(mixed, *kept):
    i32 = jnp.int32
    return pl.pallas_call(
        index_kernel,
        out_shape=[
            jax.ShapeDtypeStruct((NBLK // LANES, LANES), i32),
            jax.ShapeDtypeStruct((NBLK // LANES, LANES), i32),
            jax.ShapeDtypeStruct((WRITERS, LANES), jnp.float32),
            *[jax.ShapeDtypeStruct(k.shape, k.dtype) for k in kept],
        ],
        cost_estimate=pl.CostEstimate(flops=20_000_000, bytes_accessed=100_000, transcendentals=0),
        compiler_params=pltpu.CompilerParams(vmem_limit_bytes=8 << 20),
        name="index",
    )(mixed, *kept)


PLANES = 8
PAIR = 4


def curl_kernel(vel, xprev, xnext, yprev, ynext, zprev, znext, head, curls, mine, ends):
    comp = CX * CY
    lane = iota((CY, LANES), 1)
    row = iota((CY, LANES), 0)
    ends[...] = jnp.where(
        (lane & 1) == 0, pltpu.roll(znext[...], LANES - 1, 1), pltpu.roll(zprev[...], 1, 1)
    )
    first, last = lane == 0, lane == LANES - 1

    def plane_of(c, x):
        return vel[pl.ds(pl.multiple_of(c * comp + x * CY, CY), CY)]

    def along_x(c, x, n):
        low = jnp.maximum(x - 1, 0)
        high = jnp.minimum(x + 1, CX - 1)
        below = jnp.where(x == 0, xprev[n * CY : (n + 1) * CY], plane_of(c, low))
        above = jnp.where(x == CX - 1, xnext[n * CY : (n + 1) * CY], plane_of(c, high))
        return above - below

    def along_y(f, x, n):
        above = jnp.where(row == CY - 1, ynext[pl.ds(n * CX + x, CY, stride=0)], pltpu.roll(f, CY - 1, 0))
        below = jnp.where(row == 0, yprev[pl.ds(n * CX + x, CY, stride=0)], pltpu.roll(f, 1, 0))
        return above - below

    def along_z(f, c, x):
        edge = pltpu.roll(ends[...], LANES - 1 - 2 * (c * CX + x), 1)
        above = jnp.where(last, edge, pltpu.roll(f, LANES - 1, 1))
        below = jnp.where(first, edge, pltpu.roll(f, 1, 1))
        return above - below

    def differences(step, total):
        for p in range(PAIR):
            x = step * PAIR + p
            u, v, w = plane_of(0, x), plane_of(1, x), plane_of(2, x)
            curl = (
                along_y(w, x, 1) - along_z(v, 1, x),
                along_z(u, 0, x) - along_x(2, x, 1),
                along_x(1, x, 0) - along_y(u, x, 0),
            )
            for c in range(COMP):
                f = curl[c]
                square = f * f
                for i in range(CY // 8):
                    total += square[i * 8 : (i + 1) * 8]
                curls[pl.ds(pl.multiple_of((x * COMP + c) * CY, CY), CY)] = f
        return total

    total = lax.fori_loop(0, CX // PAIR, differences, jnp.zeros((8, LANES), jnp.float32))
    every = 0.25 * jnp.sum(total, keepdims=True)
    small = iota((8, LANES), 1)
    mine[...] = jnp.where(small == CAP, every, jnp.where(small == CAP + 1, head[0:8, :], 0.0))


def curl_of(vel2, xprev, xnext, yprev, ynext, zprev, znext, head):
    rows = COMP * NBLK
    return pl.pallas_call(
        curl_kernel,
        out_shape=[
            jax.ShapeDtypeStruct((rows, LANES), jnp.float32),
            jax.ShapeDtypeStruct((8, LANES), jnp.float32),
        ],
        scratch_shapes=[pltpu.VMEM((CY, LANES), jnp.float32)],
        cost_estimate=pl.CostEstimate(
            flops=40_000_000, bytes_accessed=7_500_000, transcendentals=0
        ),
        compiler_params=pltpu.CompilerParams(vmem_limit_bytes=16 << 20),
        name="curl",
    )(vel2, xprev, xnext, yprev, ynext, zprev, znext, head)


def transform_kernel(curls, tables, out, tiled):
    granule = iota((8, LANES), 1) >> 4
    count = PLANES * COMP

    def transform(step, carry):
        base = step * (count * CY)
        for n in range(count):
            tiles = []
            for y in range(8):
                f = curls[pl.ds(base + n * CY + (-y) % 8, 8, stride=8)]
                tiles.append(pltpu.roll(f, 16 * ((-y) % 8), 1) if y else f)
            for b in (1, 2, 4):
                moved = (granule & b) != 0
                tiles = [jnp.where(moved, tiles[(j - b) % 8], tiles[j]) for j in range(8)]
            for zb in range(8):
                tiled[zb * count * 8 + n * 8 : zb * count * 8 + n * 8 + 8] = tiles[zb]
        for zb in range(8):
            whole = tiled[zb * count * 8 : (zb + 1) * count * 8]
            high = whole.astype(jnp.bfloat16)
            low = (whole - high.astype(jnp.float32)).astype(jnp.bfloat16)
            both = jnp.dot(
                jnp.concatenate([high, low], axis=1),
                tables[zb * 256 : zb * 256 + 256],
                preferred_element_type=jnp.float32,
            )
            coeffs = both[:, :LANES] + both[:, LANES:]
            for n in range(count):
                p, c = n // COMP, n % COMP
                at = base + COMP * (p * CY + zb * 8) + c
                out[pl.ds(at, 8, stride=COMP)] = coeffs[n * 8 : n * 8 + 8]
        return carry

    lax.fori_loop(0, CX // PLANES, transform, 0)


def transform_of(curls):
    tables = jnp.asarray(tables_np())
    rows = COMP * NBLK
    return pl.pallas_call(
        transform_kernel,
        out_shape=jax.ShapeDtypeStruct((rows, LANES), jnp.float32),
        scratch_shapes=[pltpu.VMEM((PLANES * COMP * CY, LANES), jnp.float32)],
        cost_estimate=pl.CostEstimate(
            flops=2 * rows * 256 * 256, bytes_accessed=7_500_000, transcendentals=0
        ),
        compiler_params=pltpu.CompilerParams(vmem_limit_bytes=16 << 20),
        name="transform",
    )(curls, tables)


WIDTH = 2


def pack_kernel(rows, words, coeffs, head, one, two, three, four, out, room):
    lane = iota((COMP, LANES), 1)
    span, local_span = span_of(rows), room_of(rows)

    def body(r, carry):
        for j in range(WIDTH * LANES):
            p, yb, zb = j // CY, (j % CY) // 8, j % 8
            word = words[r * WIDTH + j // LANES, j % LANES]
            addr = word >> 7
            source = COMP * (p * CY + zb * 8 + yb)
            value = coeffs[pl.ds(r * (COMP * WIDTH * LANES) + source, COMP)]
            value = pltpu.roll(value, word, 1)
            kept = lane >= (jnp.full((COMP, LANES), word, jnp.int32) & (LANES - 1))
            pltpu.store(room.at[pl.ds(addr, COMP)], value, mask=kept)
            room[pl.ds(addr + COMP, COMP)] = value
        return carry

    lax.fori_loop(0, NBLK // LANES // WIDTH, body, 0)

    def settle(w, carry):
        source = pl.multiple_of(w * local_span, 8)
        target = pl.multiple_of(w * span, 8)
        out[pl.ds(target, span)] = room[pl.ds(source, span)]
        return carry

    lax.fori_loop(0, WRITERS, settle, 0)
    small = iota((8, LANES), 1)
    both = jnp.where(
        small == CAP,
        (one[...] + two[...]) + (three[...] + four[...]),
        jnp.maximum(jnp.maximum(one[...], two[...]), jnp.maximum(three[...], four[...])),
    )
    for w in range(0, WRITERS, 8):
        out[pl.ds(w * span + COMP * rows, 8, stride=span)] = jnp.where(
            small < CAP, head[w : w + 8], both
        )


def pack(words, coeffs, head, sums, rows):
    span = span_of(rows)
    return pl.pallas_call(
        functools.partial(pack_kernel, rows),
        in_specs=[
            pl.BlockSpec(memory_space=pltpu.SMEM),
            *[pl.BlockSpec(memory_space=pltpu.VMEM)] * 6,
        ],
        out_specs=pl.BlockSpec(memory_space=pltpu.VMEM),
        out_shape=jax.ShapeDtypeStruct((WRITERS * span, LANES), jnp.float32),
        scratch_shapes=[pltpu.VMEM((WRITERS * room_of(rows), LANES), jnp.float32)],
        cost_estimate=pl.CostEstimate(
            flops=200_000_000, bytes_accessed=8_000_000, transcendentals=0
        ),
        compiler_params=pltpu.CompilerParams(vmem_limit_bytes=22 << 20),
    )(words, coeffs, head, *sums)


SOURCES = 8
ABREAST = 8


def unpack_kernel(rows, *refs):
    head = None
    if len(refs) == 10:
        head, refs = refs[0], refs[1:]
    recv, out, spill, heads, words_s, words_v, scale, pieces, sem = refs
    step = pl.program_id(0)
    span = span_of(rows)

    @pl.when(step == 0)
    def _():
        if head is None:
            h = recv[pl.ds(COMP * rows, WRITERS, stride=span)]
        else:
            h = head[...]
        heads[...] = h
        lane = iota((WRITERS, LANES), 1)
        lens = jnp.where(lane < CAP, h, 0.0)
        before = (iota((LANES, LANES), 0) < iota((LANES, LANES), 1)).astype(jnp.bfloat16)
        start = jnp.dot(lens.astype(jnp.bfloat16), before, preferred_element_type=jnp.float32)
        start = start.astype(jnp.int32)
        first = start >> 7
        turn = start & (LANES - 1)
        at = iota((WRITERS, LANES), 0) * span + COMP * jnp.minimum(first, rows - 2)
        late = (first >= rows - 1).astype(jnp.int32)
        words_v[...] = (
            (at << 17) + (lens.astype(jnp.int32) << 9) + (late << 8) + (LANES - turn)
        )
        copy = pltpu.make_async_copy(words_v, words_s, sem)
        copy.start()
        total = jnp.sum(jnp.where(lane == CAP, h, 0.0), keepdims=True)
        rms = jnp.sqrt(total * (1.0 / CELLS) + 1e-6)
        scale[...] = jnp.broadcast_to(1.0 / rms, scale.shape)
        spill[0, 0] = jnp.max(jnp.where(lane == CAP + 1, h, 0.0)).astype(jnp.int32)
        copy.wait()

    factor = scale[...]
    lane = iota((COMP, LANES), 1)

    def body(s, carry):
        for k in range(ABREAST * CAP):
            number, q = step * SOURCES + s * ABREAST + k // CAP, k % CAP
            word = words_s[number, q]
            marks = jnp.full((COMP, LANES), word, jnp.int32)
            at = word >> 17
            one = recv[pl.ds(at, COMP)]
            two = recv[pl.ds(at + COMP, COMP)]
            inside = ((marks & 511) + lane) & 384
            value = jnp.where(inside == LANES, one, two)
            value = pltpu.roll(value, word, 1)
            value = jnp.where(lane < ((marks >> 9) & 255), value, 0.0)
            pieces[k * 4 : k * 4 + COMP] = value
        for k in range(0, ABREAST * CAP, 8):
            for c in range(COMP):
                row = pl.multiple_of(s * (ABREAST * CAP) + k, 8)
                out[c, pl.ds(row, 8)] = pieces[pl.ds(k * 4 + c, 8, stride=4)] * factor
        return carry

    lax.fori_loop(0, SOURCES // ABREAST, body, 0)


def unpack(recv, rows, head=None):
    args = (recv,) if head is None else (head, recv)
    return pl.pallas_call(
        functools.partial(unpack_kernel, rows),
        grid=(WRITERS // SOURCES,),
        in_specs=[pl.BlockSpec(a.shape, lambda i: (0, 0)) for a in args],
        out_specs=[
            pl.BlockSpec((COMP, SOURCES * CAP, LANES), lambda i: (0, i, 0)),
            pl.BlockSpec(memory_space=pltpu.SMEM),
            pl.BlockSpec((WRITERS, LANES), lambda i: (0, 0)),
        ],
        out_shape=[
            jax.ShapeDtypeStruct((COMP, WRITERS * CAP, LANES), jnp.float32),
            jax.ShapeDtypeStruct((1, 1), jnp.int32),
            jax.ShapeDtypeStruct((WRITERS, LANES), jnp.float32),
        ],
        scratch_shapes=[
            pltpu.SMEM((WRITERS, LANES), jnp.int32),
            pltpu.VMEM((WRITERS, LANES), jnp.int32),
            pltpu.VMEM((8, LANES), jnp.float32),
            pltpu.VMEM((ABREAST * CAP * 4, LANES), jnp.float32),
            pltpu.SemaphoreType.DMA,
        ],
        cost_estimate=pl.CostEstimate(
            flops=200_000_000, bytes_accessed=11_000_000, transcendentals=0
        ),
        compiler_params=pltpu.CompilerParams(vmem_limit_bytes=24 << 20),
    )(*args)


def exchange(buffer, rows):
    return lax.all_to_all(
        buffer.reshape(WRITERS, span_of(rows), LANES), G, 0, 0, tiled=True
    )


def body_of(velocity, lengths, destinations):
    vel2 = velocity.reshape(COMP * CX * CY, LANES)
    mixed = (destinations * 256 + lengths.reshape(destinations.shape)).reshape(NBLK // LANES, LANES)

    xlo, xhi, ylo, yhi, zt, vel2 = faces(vel2)

    def ring(axis, n, d):
        return functools.partial(
            lax.ppermute, axis_name=axis, perm=[(i, (i + d) % n) for i in range(n)]
        )

    n_x, n_y, n_z = (lax.axis_size(a) for a in ("gx", "gy", "wa"))
    xprev, xnext = ring("gx", n_x, 1)(xhi), ring("gx", n_x, -1)(xlo)
    words, wide, head, ylo, yhi, zt = index(mixed, ylo, yhi, zt)
    yprev, ynext = ring("gy", n_y, 1)(yhi), ring("gy", n_y, -1)(ylo)
    zprev, znext = ring("wa", n_z, 1)(zt), ring("wa", n_z, -1)(zt)

    curls, mine = curl_of(vel2, xprev, xnext, yprev, ynext, zprev, znext, head)
    sums = [mine] + [ring("wa", n_z, d)(mine) for d in range(1, n_z)]
    coeffs = transform_of(curls)
    packed = pack(words, coeffs, head, sums, ROWS)
    got = exchange(packed, ROWS)
    out, spill, heads = unpack(got.reshape(-1, LANES), ROWS)

    def again(carry):
        more = exchange(pack(wide, coeffs, head, sums, CAP), CAP)
        wider, _, _ = unpack(more.reshape(-1, LANES), CAP, heads)
        return jnp.int32(0), wider

    _, out = lax.while_loop(lambda carry: carry[0] > 0, again, (spill.reshape(()), out))
    return out.reshape(1, 1, COMP, WRITERS, CAP, LANES)


def solution(mesh):
    return jax.shard_map(
        body_of,
        mesh=mesh,
        in_specs=(
            P(None, "gx", "gy", "wa"),
            P("gx", "gy", "wa", None),
            P("gx", "gy", "wa", None, None),
        ),
        out_specs=P(G, "wa", None, None, None, None),
        check_vma=False,
    )
```

```python
import functools

import jax
import jax.numpy as jnp
import numpy as np
from jax import lax
from jax.experimental import pallas as pl
from jax.experimental.pallas import tpu as pltpu
from jax.sharding import PartitionSpec as P

BY = 8
BZ = 16
LANES = 128
COMP = 3
CX = 32
CY = 64
NBLK = 2048
WRITERS = 64
CAP = 64
ROWS = 45
CELLS = 256 * 512 * 512 * 3
G = ("gx", "gy")


def span_of(rows):
    return -(-(COMP * rows + 1) // 8) * 8


def room_of(rows):
    return -(-(COMP * rows + 6) // 8) * 8


def dct_np(n):
    k = np.arange(n, dtype=np.float64)[:, None]
    j = np.arange(n, dtype=np.float64)[None, :]
    t = np.sqrt(2.0 / n) * np.cos(np.pi * (j + 0.5) * k / n)
    t[0] *= np.sqrt(0.5)
    return t


def tables_np():
    k = (0.5 * np.kron(dct_np(BY), dct_np(BZ)).T).astype(np.float32)
    high = k.astype(jnp.bfloat16)
    low = (k - high.astype(np.float32)).astype(jnp.bfloat16)
    top = np.concatenate([high, low], axis=1)
    bottom = np.concatenate([high, np.zeros_like(low)], axis=1)
    turned = [np.concatenate([np.roll(part, BZ * zb, axis=0) for part in (top, bottom)]) for zb in range(8)]
    return np.concatenate(turned, axis=0)


def iota(shape, dim):
    return lax.broadcasted_iota(jnp.int32, shape, dim)


def faces_kernel(vel, xlo, xhi, ylo, yhi, zt, held):
    plane = CY
    comp = CX * CY
    for n, c in enumerate((1, 2)):
        xlo[n * plane : (n + 1) * plane] = vel[c * comp : c * comp + plane]
        xhi[n * plane : (n + 1) * plane] = vel[(c + 1) * comp - plane : (c + 1) * comp]
    for n, c in enumerate((0, 2)):
        ylo[n * CX : (n + 1) * CX] = vel[pl.ds(c * comp, CX, stride=plane)]
        yhi[n * CX : (n + 1) * CX] = vel[pl.ds(c * comp + plane - 1, CX, stride=plane)]
    lane = iota((CY, LANES), 1)
    t = jnp.zeros((CY, LANES), jnp.float32)
    for k in range(2 * CX):
        f = vel[k * plane : (k + 1) * plane]
        t = jnp.where((lane >> 1) == k, pltpu.roll(f, (2 * k + 1) % LANES, 1), t)
    zt[...] = t
    held[...] = vel[...]


def faces(vel2):
    f32 = jnp.float32
    return pl.pallas_call(
        faces_kernel,
        out_shape=[
            jax.ShapeDtypeStruct((2 * CY, LANES), f32),
            jax.ShapeDtypeStruct((2 * CY, LANES), f32),
            jax.ShapeDtypeStruct((2 * CX, LANES), f32),
            jax.ShapeDtypeStruct((2 * CX, LANES), f32),
            jax.ShapeDtypeStruct((CY, LANES), f32),
            jax.ShapeDtypeStruct(vel2.shape, f32),
        ],
        cost_estimate=pl.CostEstimate(flops=4_000_000, bytes_accessed=3_500_000, transcendentals=0),
        compiler_params=pltpu.CompilerParams(vmem_limit_bytes=10 << 20),
        name="faces",
    )(vel2)


def index_kernel(mixed, words, wide, head):
    chunks = NBLK // LANES
    t = mixed[...] >> 8
    ln = mixed[...] & 255
    row = iota((WRITERS, LANES), 0)
    before = (iota((LANES, LANES), 0) < iota((LANES, LANES), 1)).astype(jnp.bfloat16)
    ones = jnp.ones((LANES, LANES), jnp.bfloat16)
    rhs = jnp.concatenate([before, ones], axis=1)
    hits, weighted = [], []
    for r in range(chunks):
        hit = t[r : r + 1, :] == row
        hits.append(hit)
        weighted.append(jnp.where(hit, ln[r : r + 1, :], 0).astype(jnp.float32).astype(jnp.bfloat16))
    counted = [jnp.where(h, 1.0, 0.0).astype(jnp.bfloat16) for h in hits]
    nt = (((1,), (1,)), ((), ()))
    base_l = jnp.zeros((WRITERS, LANES), jnp.float32)
    base_c = jnp.zeros((WRITERS, LANES), jnp.float32)
    lens = jnp.zeros((WRITERS, LANES), jnp.float32)
    starts = []
    for r in range(chunks):
        sums_l = jnp.dot(weighted[r], rhs, preferred_element_type=jnp.float32)
        sums_c = jnp.dot(counted[r], rhs, preferred_element_type=jnp.float32)
        start = jnp.where(hits[r], sums_l[:, :LANES] + base_l, 0.0)
        rank = jnp.where(hits[r], sums_c[:, :LANES] + base_c, 0.0)
        starts.append(jnp.sum(start, axis=0, keepdims=True))
        slot = jnp.sum(rank, axis=0, keepdims=True).astype(jnp.int32)
        at = jnp.where(slot == iota((LANES, LANES), 0), 1.0, 0.0).astype(jnp.bfloat16)
        lens += lax.dot_general(weighted[r], at, nt, preferred_element_type=jnp.float32)
        base_l += sums_l[:, LANES:]
        base_c += sums_c[:, LANES:]
    start = jnp.concatenate(starts, axis=0).astype(jnp.int32)
    first = start >> 7
    shift = start & (LANES - 1)
    words[...] = (t * room_of(ROWS) + COMP * jnp.minimum(first, ROWS)) * LANES + shift
    wide[...] = (t * room_of(CAP) + COMP * jnp.minimum(first, CAP)) * LANES + shift
    full = jnp.max(base_l, axis=0, keepdims=True)
    spill = jnp.where(full > ROWS * LANES, 1.0, 0.0)
    lane = iota((WRITERS, LANES), 1)
    head[...] = jnp.where(lane < CAP, lens, jnp.where(lane == CAP + 1, spill, 0.0))


def index(mixed):
    i32 = jnp.int32
    return pl.pallas_call(
        index_kernel,
        out_shape=[
            jax.ShapeDtypeStruct((NBLK // LANES, LANES), i32),
            jax.ShapeDtypeStruct((NBLK // LANES, LANES), i32),
            jax.ShapeDtypeStruct((WRITERS, LANES), jnp.float32),
        ],
        cost_estimate=pl.CostEstimate(flops=20_000_000, bytes_accessed=100_000, transcendentals=0),
        compiler_params=pltpu.CompilerParams(vmem_limit_bytes=8 << 20),
        name="index",
    )(mixed)


PLANES = 32
PAIR = 16


def curl_kernel(vel, xprev, xnext, yprev, ynext, zprev, znext, head, curls, mine, ends):
    comp = CX * CY
    lane = iota((CY, LANES), 1)
    row = iota((CY, LANES), 0)
    ends[...] = jnp.where(
        (lane & 1) == 0, pltpu.roll(znext[...], LANES - 1, 1), pltpu.roll(zprev[...], 1, 1)
    )
    first, last = lane == 0, lane == LANES - 1

    def plane_of(c, x):
        return vel[pl.ds(pl.multiple_of(c * comp + x * CY, CY), CY)]

    def along_x(c, x, n):
        low = jnp.maximum(x - 1, 0)
        high = jnp.minimum(x + 1, CX - 1)
        below = jnp.where(x == 0, xprev[n * CY : (n + 1) * CY], plane_of(c, low))
        above = jnp.where(x == CX - 1, xnext[n * CY : (n + 1) * CY], plane_of(c, high))
        return above - below

    def along_y(f, x, n):
        above = jnp.where(row == CY - 1, ynext[pl.ds(n * CX + x, CY, stride=0)], pltpu.roll(f, CY - 1, 0))
        below = jnp.where(row == 0, yprev[pl.ds(n * CX + x, CY, stride=0)], pltpu.roll(f, 1, 0))
        return above - below

    def along_z(f, c, x):
        edge = pltpu.roll(ends[...], LANES - 1 - 2 * (c * CX + x), 1)
        above = jnp.where(last, edge, pltpu.roll(f, LANES - 1, 1))
        below = jnp.where(first, edge, pltpu.roll(f, 1, 1))
        return above - below

    def differences(step, total):
        for p in range(PAIR):
            x = step * PAIR + p
            u, v, w = plane_of(0, x), plane_of(1, x), plane_of(2, x)
            curl = (
                along_y(w, x, 1) - along_z(v, 1, x),
                along_z(u, 0, x) - along_x(2, x, 1),
                along_x(1, x, 0) - along_y(u, x, 0),
            )
            for c in range(COMP):
                f = curl[c]
                square = f * f
                for i in range(CY // 8):
                    total += square[i * 8 : (i + 1) * 8]
                curls[pl.ds(pl.multiple_of((x * COMP + c) * CY, CY), CY)] = f
        return total

    total = lax.fori_loop(0, CX // PAIR, differences, jnp.zeros((8, LANES), jnp.float32))
    every = 0.25 * jnp.sum(total, keepdims=True)
    small = iota((8, LANES), 1)
    mine[...] = jnp.where(small == CAP, every, jnp.where(small == CAP + 1, head[0:8, :], 0.0))


def curl_of(vel2, xprev, xnext, yprev, ynext, zprev, znext, head):
    rows = COMP * NBLK
    return pl.pallas_call(
        curl_kernel,
        out_shape=[
            jax.ShapeDtypeStruct((rows, LANES), jnp.float32),
            jax.ShapeDtypeStruct((8, LANES), jnp.float32),
        ],
        scratch_shapes=[pltpu.VMEM((CY, LANES), jnp.float32)],
        cost_estimate=pl.CostEstimate(
            flops=40_000_000, bytes_accessed=7_500_000, transcendentals=0
        ),
        compiler_params=pltpu.CompilerParams(vmem_limit_bytes=16 << 20),
        name="curl",
    )(vel2, xprev, xnext, yprev, ynext, zprev, znext, head)


def transform_kernel(curls, tables, out, tiled):
    granule = iota((8, LANES), 1) >> 4
    count = PLANES * COMP

    def transform(step, carry):
        base = step * (count * CY)
        for n in range(count):
            tiles = []
            for y in range(8):
                f = curls[pl.ds(base + n * CY + (-y) % 8, 8, stride=8)]
                tiles.append(pltpu.roll(f, 16 * ((-y) % 8), 1) if y else f)
            for b in (1, 2, 4):
                moved = (granule & b) != 0
                tiles = [jnp.where(moved, tiles[(j - b) % 8], tiles[j]) for j in range(8)]
            for zb in range(8):
                tiled[zb * count * 8 + n * 8 : zb * count * 8 + n * 8 + 8] = tiles[zb]
        for zb in range(8):
            whole = tiled[zb * count * 8 : (zb + 1) * count * 8]
            high = whole.astype(jnp.bfloat16)
            low = (whole - high.astype(jnp.float32)).astype(jnp.bfloat16)
            both = jnp.dot(
                jnp.concatenate([high, low], axis=1),
                tables[zb * 256 : zb * 256 + 256],
                preferred_element_type=jnp.float32,
            )
            coeffs = both[:, :LANES] + both[:, LANES:]
            for n in range(count):
                p, c = n // COMP, n % COMP
                at = base + COMP * (p * CY + zb * 8) + c
                out[pl.ds(at, 8, stride=COMP)] = coeffs[n * 8 : n * 8 + 8]
        return carry

    lax.fori_loop(0, CX // PLANES, transform, 0)


def transform_of(curls):
    tables = jnp.asarray(tables_np())
    rows = COMP * NBLK
    return pl.pallas_call(
        transform_kernel,
        out_shape=jax.ShapeDtypeStruct((rows, LANES), jnp.float32),
        scratch_shapes=[pltpu.VMEM((PLANES * COMP * CY, LANES), jnp.float32)],
        cost_estimate=pl.CostEstimate(
            flops=2 * rows * 256 * 256, bytes_accessed=7_500_000, transcendentals=0
        ),
        compiler_params=pltpu.CompilerParams(vmem_limit_bytes=16 << 20),
        name="transform",
    )(curls, tables)


WIDTH = 4


def pack_kernel(rows, words, coeffs, head, one, two, three, four, out, room):
    lane = iota((COMP, LANES), 1)
    span, local_span = span_of(rows), room_of(rows)

    def body(r, carry):
        for j in range(WIDTH * LANES):
            p, yb, zb = j // CY, (j % CY) // 8, j % 8
            word = words[r * WIDTH + j // LANES, j % LANES]
            addr = word >> 7
            source = COMP * (p * CY + zb * 8 + yb)
            value = coeffs[pl.ds(r * (COMP * WIDTH * LANES) + source, COMP)]
            value = pltpu.roll(value, word, 1)
            kept = lane >= (jnp.full((COMP, LANES), word, jnp.int32) & (LANES - 1))
            pltpu.store(room.at[pl.ds(addr, COMP)], value, mask=kept)
            room[pl.ds(addr + COMP, COMP)] = value
        return carry

    lax.fori_loop(0, NBLK // LANES // WIDTH, body, 0)

    def settle(w, carry):
        for k in range(8):
            source = pl.multiple_of((w * 8 + k) * local_span, 8)
            target = pl.multiple_of((w * 8 + k) * span, 8)
            out[pl.ds(target, span)] = room[pl.ds(source, span)]
        return carry

    lax.fori_loop(0, WRITERS // 8, settle, 0)
    small = iota((8, LANES), 1)
    both = jnp.where(
        small == CAP,
        (one[...] + two[...]) + (three[...] + four[...]),
        jnp.maximum(jnp.maximum(one[...], two[...]), jnp.maximum(three[...], four[...])),
    )
    for w in range(0, WRITERS, 8):
        out[pl.ds(w * span + COMP * rows, 8, stride=span)] = jnp.where(
            small < CAP, head[w : w + 8], both
        )


def pack(words, coeffs, head, sums, rows):
    span = span_of(rows)
    return pl.pallas_call(
        functools.partial(pack_kernel, rows),
        in_specs=[
            pl.BlockSpec(memory_space=pltpu.SMEM),
            *[pl.BlockSpec(memory_space=pltpu.VMEM)] * 6,
        ],
        out_specs=pl.BlockSpec(memory_space=pltpu.VMEM),
        out_shape=jax.ShapeDtypeStruct((WRITERS * span, LANES), jnp.float32),
        scratch_shapes=[pltpu.VMEM((WRITERS * room_of(rows), LANES), jnp.float32)],
        cost_estimate=pl.CostEstimate(
            flops=200_000_000, bytes_accessed=8_000_000, transcendentals=0
        ),
        compiler_params=pltpu.CompilerParams(vmem_limit_bytes=22 << 20),
        name=f"pack{rows}",
    )(words, coeffs, head, *sums)


SOURCES = 8
ABREAST = 8


def unpack_kernel(rows, *refs):
    head = None
    if len(refs) == 10:
        head, refs = refs[0], refs[1:]
    recv, out, spill, heads, words_s, words_v, scale, pieces, sem = refs
    step = pl.program_id(0)
    span = span_of(rows)

    @pl.when(step == 0)
    def _():
        if head is None:
            h = recv[pl.ds(COMP * rows, WRITERS, stride=span)]
        else:
            h = head[...]
        heads[...] = h
        lane = iota((WRITERS, LANES), 1)
        lens = jnp.where(lane < CAP, h, 0.0)
        before = (iota((LANES, LANES), 0) < iota((LANES, LANES), 1)).astype(jnp.bfloat16)
        start = jnp.dot(lens.astype(jnp.bfloat16), before, preferred_element_type=jnp.float32)
        start = start.astype(jnp.int32)
        first = start >> 7
        turn = start & (LANES - 1)
        at = iota((WRITERS, LANES), 0) * span + COMP * jnp.minimum(first, rows - 2)
        late = (first >= rows - 1).astype(jnp.int32)
        words_v[...] = (
            (at << 17) + (lens.astype(jnp.int32) << 9) + (late << 8) + (LANES - turn)
        )
        copy = pltpu.make_async_copy(words_v, words_s, sem)
        copy.start()
        total = jnp.sum(jnp.where(lane == CAP, h, 0.0), keepdims=True)
        rms = jnp.sqrt(total * (1.0 / CELLS) + 1e-6)
        scale[...] = jnp.broadcast_to(1.0 / rms, scale.shape)
        spill[0, 0] = jnp.max(jnp.where(lane == CAP + 1, h, 0.0)).astype(jnp.int32)
        copy.wait()

    factor = scale[...]
    lane = iota((COMP, LANES), 1)

    def body(s, carry):
        for k in range(ABREAST * CAP):
            number, q = step * SOURCES + s * ABREAST + k // CAP, k % CAP
            word = words_s[number, q]
            marks = jnp.full((COMP, LANES), word, jnp.int32)
            at = word >> 17
            one = recv[pl.ds(at, COMP)]
            two = recv[pl.ds(at + COMP, COMP)]
            inside = ((marks & 511) + lane) & 384
            value = jnp.where(inside == LANES, one, two)
            value = pltpu.roll(value, word, 1)
            value = jnp.where(lane < ((marks >> 9) & 255), value, 0.0)
            pieces[k * 4 : k * 4 + COMP] = value
        for k in range(0, ABREAST * CAP, 8):
            for c in range(COMP):
                row = pl.multiple_of(s * (ABREAST * CAP) + k, 8)
                out[c, pl.ds(row, 8)] = pieces[pl.ds(k * 4 + c, 8, stride=4)] * factor
        return carry

    lax.fori_loop(0, SOURCES // ABREAST, body, 0)


def unpack(recv, rows, head=None):
    args = (recv,) if head is None else (head, recv)
    return pl.pallas_call(
        functools.partial(unpack_kernel, rows),
        grid=(WRITERS // SOURCES,),
        in_specs=[pl.BlockSpec(a.shape, lambda i: (0, 0)) for a in args],
        out_specs=[
            pl.BlockSpec((COMP, SOURCES * CAP, LANES), lambda i: (0, i, 0)),
            pl.BlockSpec(memory_space=pltpu.SMEM),
            pl.BlockSpec((WRITERS, LANES), lambda i: (0, 0)),
        ],
        out_shape=[
            jax.ShapeDtypeStruct((COMP, WRITERS * CAP, LANES), jnp.float32),
            jax.ShapeDtypeStruct((1, 1), jnp.int32),
            jax.ShapeDtypeStruct((WRITERS, LANES), jnp.float32),
        ],
        scratch_shapes=[
            pltpu.SMEM((WRITERS, LANES), jnp.int32),
            pltpu.VMEM((WRITERS, LANES), jnp.int32),
            pltpu.VMEM((8, LANES), jnp.float32),
            pltpu.VMEM((ABREAST * CAP * 4, LANES), jnp.float32),
            pltpu.SemaphoreType.DMA,
        ],
        cost_estimate=pl.CostEstimate(
            flops=200_000_000, bytes_accessed=11_000_000, transcendentals=0
        ),
        compiler_params=pltpu.CompilerParams(vmem_limit_bytes=24 << 20),
        name=f"unpack{rows}",
    )(*args)


def exchange(buffer, rows):
    return lax.all_to_all(
        buffer.reshape(WRITERS, span_of(rows), LANES), G, 0, 0, tiled=True
    )


def local(velocity, lengths, destinations):
    vel2 = velocity.reshape(COMP * CX * CY, LANES)
    mixed = (destinations * 256 + lengths.reshape(destinations.shape)).reshape(NBLK // LANES, LANES)

    xlo, xhi, ylo, yhi, zt, vel2 = faces(vel2)

    def ring(axis, n, d):
        return functools.partial(
            lax.ppermute, axis_name=axis, perm=[(i, (i + d) % n) for i in range(n)]
        )

    n_x, n_y, n_z = (lax.axis_size(a) for a in ("gx", "gy", "wa"))
    xprev, xnext = ring("gx", n_x, 1)(xhi), ring("gx", n_x, -1)(xlo)
    yprev, ynext = ring("gy", n_y, 1)(yhi), ring("gy", n_y, -1)(ylo)
    zprev, znext = ring("wa", n_z, 1)(zt), ring("wa", n_z, -1)(zt)
    words, wide, head = index(mixed)

    curls, mine = curl_of(vel2, xprev, xnext, yprev, ynext, zprev, znext, head)
    sums = [mine] + [ring("wa", n_z, d)(mine) for d in range(1, n_z)]
    coeffs = transform_of(curls)
    packed = pack(words, coeffs, head, sums, ROWS)
    got = exchange(packed, ROWS)
    out, spill, heads = unpack(got.reshape(-1, LANES), ROWS)

    def again(carry):
        more = exchange(pack(wide, coeffs, head, sums, CAP), CAP)
        wider, _, _ = unpack(more.reshape(-1, LANES), CAP, heads)
        return jnp.int32(0), wider

    _, out = lax.while_loop(lambda carry: carry[0] > 0, again, (spill.reshape(()), out))
    return out.reshape(1, 1, COMP, WRITERS, CAP, LANES)


def solution(mesh):
    return jax.shard_map(
        local,
        mesh=mesh,
        in_specs=(
            P(None, "gx", "gy", "wa"),
            P("gx", "gy", "wa", None),
            P("gx", "gy", "wa", None, None),
        ),
        out_specs=P(G, "wa", None, None, None, None),
        check_vma=False,
    )
```

```python
import functools

import jax
import jax.numpy as jnp
import numpy as np
from jax import lax
from jax.experimental import pallas as pl
from jax.experimental.pallas import tpu as pltpu
from jax.sharding import PartitionSpec as P

BY = 8
BZ = 16
LANES = 128
COMP = 3
CX = 32
CY = 64
NBLK = 2048
WRITERS = 64
CAP = 64
ROWS = 45
CELLS = 256 * 512 * 512 * 3
G = ("gx", "gy")


def span_of(rows):
    return -(-(COMP * rows + 1) // 8) * 8


def room_of(rows):
    return -(-(COMP * rows + 6) // 8) * 8


def dct_np(n):
    k = np.arange(n, dtype=np.float64)[:, None]
    j = np.arange(n, dtype=np.float64)[None, :]
    t = np.sqrt(2.0 / n) * np.cos(np.pi * (j + 0.5) * k / n)
    t[0] *= np.sqrt(0.5)
    return t


def tables_np():
    k = (0.5 * np.kron(dct_np(BY), dct_np(BZ)).T).astype(np.float32)
    high = k.astype(jnp.bfloat16)
    low = (k - high.astype(np.float32)).astype(jnp.bfloat16)
    top = np.concatenate([high, low], axis=1)
    bottom = np.concatenate([high, np.zeros_like(low)], axis=1)
    turned = [np.concatenate([np.roll(part, BZ * zb, axis=0) for part in (top, bottom)]) for zb in range(8)]
    return np.concatenate(turned, axis=0)


def iota(shape, dim):
    return lax.broadcasted_iota(jnp.int32, shape, dim)


def faces_kernel(vel, xlo, xhi, ylo, yhi, zt, held):
    plane = CY
    comp = CX * CY
    for n, c in enumerate((1, 2)):
        xlo[n * plane : (n + 1) * plane] = vel[c * comp : c * comp + plane]
        xhi[n * plane : (n + 1) * plane] = vel[(c + 1) * comp - plane : (c + 1) * comp]
    for n, c in enumerate((0, 2)):
        ylo[n * CX : (n + 1) * CX] = vel[pl.ds(c * comp, CX, stride=plane)]
        yhi[n * CX : (n + 1) * CX] = vel[pl.ds(c * comp + plane - 1, CX, stride=plane)]
    lane = iota((CY, LANES), 1)
    t = jnp.zeros((CY, LANES), jnp.float32)
    for k in range(2 * CX):
        f = vel[k * plane : (k + 1) * plane]
        t = jnp.where((lane >> 1) == k, pltpu.roll(f, (2 * k + 1) % LANES, 1), t)
    zt[...] = t
    held[...] = vel[...]


def faces(vel2):
    f32 = jnp.float32
    return pl.pallas_call(
        faces_kernel,
        out_shape=[
            jax.ShapeDtypeStruct((2 * CY, LANES), f32),
            jax.ShapeDtypeStruct((2 * CY, LANES), f32),
            jax.ShapeDtypeStruct((2 * CX, LANES), f32),
            jax.ShapeDtypeStruct((2 * CX, LANES), f32),
            jax.ShapeDtypeStruct((CY, LANES), f32),
            jax.ShapeDtypeStruct(vel2.shape, f32),
        ],
        cost_estimate=pl.CostEstimate(flops=4_000_000, bytes_accessed=3_500_000, transcendentals=0),
        compiler_params=pltpu.CompilerParams(vmem_limit_bytes=10 << 20),
        name="faces",
    )(vel2)


def index_kernel(mixed, words, wide, head):
    chunks = NBLK // LANES
    t = mixed[...] >> 8
    ln = mixed[...] & 255
    row = iota((WRITERS, LANES), 0)
    before = (iota((LANES, LANES), 0) < iota((LANES, LANES), 1)).astype(jnp.bfloat16)
    ones = jnp.ones((LANES, LANES), jnp.bfloat16)
    rhs = jnp.concatenate([before, ones], axis=1)
    hits, weighted = [], []
    for r in range(chunks):
        hit = t[r : r + 1, :] == row
        hits.append(hit)
        weighted.append(jnp.where(hit, ln[r : r + 1, :], 0).astype(jnp.float32).astype(jnp.bfloat16))
    counted = [jnp.where(h, 1.0, 0.0).astype(jnp.bfloat16) for h in hits]
    nt = (((1,), (1,)), ((), ()))
    base_l = jnp.zeros((WRITERS, LANES), jnp.float32)
    base_c = jnp.zeros((WRITERS, LANES), jnp.float32)
    lens = jnp.zeros((WRITERS, LANES), jnp.float32)
    starts = []
    for r in range(chunks):
        sums_l = jnp.dot(weighted[r], rhs, preferred_element_type=jnp.float32)
        sums_c = jnp.dot(counted[r], rhs, preferred_element_type=jnp.float32)
        start = jnp.where(hits[r], sums_l[:, :LANES] + base_l, 0.0)
        rank = jnp.where(hits[r], sums_c[:, :LANES] + base_c, 0.0)
        starts.append(jnp.sum(start, axis=0, keepdims=True))
        slot = jnp.sum(rank, axis=0, keepdims=True).astype(jnp.int32)
        at = jnp.where(slot == iota((LANES, LANES), 0), 1.0, 0.0).astype(jnp.bfloat16)
        lens += lax.dot_general(weighted[r], at, nt, preferred_element_type=jnp.float32)
        base_l += sums_l[:, LANES:]
        base_c += sums_c[:, LANES:]
    start = jnp.concatenate(starts, axis=0).astype(jnp.int32)
    first = start >> 7
    shift = start & (LANES - 1)
    words[...] = (t * room_of(ROWS) + COMP * jnp.minimum(first, ROWS)) * LANES + shift
    wide[...] = (t * room_of(CAP) + COMP * jnp.minimum(first, CAP)) * LANES + shift
    full = jnp.max(base_l, axis=0, keepdims=True)
    spill = jnp.where(full > ROWS * LANES, 1.0, 0.0)
    lane = iota((WRITERS, LANES), 1)
    head[...] = jnp.where(lane < CAP, lens, jnp.where(lane == CAP + 1, spill, 0.0))


def index(mixed):
    i32 = jnp.int32
    return pl.pallas_call(
        index_kernel,
        out_shape=[
            jax.ShapeDtypeStruct((NBLK // LANES, LANES), i32),
            jax.ShapeDtypeStruct((NBLK // LANES, LANES), i32),
            jax.ShapeDtypeStruct((WRITERS, LANES), jnp.float32),
        ],
        cost_estimate=pl.CostEstimate(flops=20_000_000, bytes_accessed=100_000, transcendentals=0),
        compiler_params=pltpu.CompilerParams(vmem_limit_bytes=8 << 20),
        name="index",
    )(mixed)


PLANES = 32
PAIR = 32


def curl_kernel(vel, xprev, xnext, yprev, ynext, zprev, znext, head, curls, mine, ends):
    comp = CX * CY
    lane = iota((CY, LANES), 1)
    row = iota((CY, LANES), 0)
    ends[...] = jnp.where(
        (lane & 1) == 0, pltpu.roll(znext[...], LANES - 1, 1), pltpu.roll(zprev[...], 1, 1)
    )
    first, last = lane == 0, lane == LANES - 1

    def plane_of(c, x):
        return vel[pl.ds(pl.multiple_of(c * comp + x * CY, CY), CY)]

    def along_x(c, x, n):
        low = jnp.maximum(x - 1, 0)
        high = jnp.minimum(x + 1, CX - 1)
        below = jnp.where(x == 0, xprev[n * CY : (n + 1) * CY], plane_of(c, low))
        above = jnp.where(x == CX - 1, xnext[n * CY : (n + 1) * CY], plane_of(c, high))
        return above - below

    def along_y(f, x, n):
        above = jnp.where(row == CY - 1, ynext[pl.ds(n * CX + x, CY, stride=0)], pltpu.roll(f, CY - 1, 0))
        below = jnp.where(row == 0, yprev[pl.ds(n * CX + x, CY, stride=0)], pltpu.roll(f, 1, 0))
        return above - below

    def along_z(f, c, x):
        edge = pltpu.roll(ends[...], LANES - 1 - 2 * (c * CX + x), 1)
        above = jnp.where(last, edge, pltpu.roll(f, LANES - 1, 1))
        below = jnp.where(first, edge, pltpu.roll(f, 1, 1))
        return above - below

    def differences(step, total):
        for p in range(PAIR):
            x = step * PAIR + p
            u, v, w = plane_of(0, x), plane_of(1, x), plane_of(2, x)
            curl = (
                along_y(w, x, 1) - along_z(v, 1, x),
                along_z(u, 0, x) - along_x(2, x, 1),
                along_x(1, x, 0) - along_y(u, x, 0),
            )
            for c in range(COMP):
                f = curl[c]
                square = f * f
                for i in range(CY // 8):
                    total += square[i * 8 : (i + 1) * 8]
                curls[pl.ds(pl.multiple_of((x * COMP + c) * CY, CY), CY)] = f
        return total

    total = lax.fori_loop(0, CX // PAIR, differences, jnp.zeros((8, LANES), jnp.float32))
    every = 0.25 * jnp.sum(total, keepdims=True)
    small = iota((8, LANES), 1)
    mine[...] = jnp.where(small == CAP, every, jnp.where(small == CAP + 1, head[0:8, :], 0.0))


def curl_of(vel2, xprev, xnext, yprev, ynext, zprev, znext, head):
    rows = COMP * NBLK
    return pl.pallas_call(
        curl_kernel,
        out_shape=[
            jax.ShapeDtypeStruct((rows, LANES), jnp.float32),
            jax.ShapeDtypeStruct((8, LANES), jnp.float32),
        ],
        scratch_shapes=[pltpu.VMEM((CY, LANES), jnp.float32)],
        cost_estimate=pl.CostEstimate(
            flops=40_000_000, bytes_accessed=7_500_000, transcendentals=0
        ),
        compiler_params=pltpu.CompilerParams(vmem_limit_bytes=16 << 20),
        name="curl",
    )(vel2, xprev, xnext, yprev, ynext, zprev, znext, head)


def transform_kernel(curls, tables, out, tiled):
    granule = iota((8, LANES), 1) >> 4
    count = PLANES * COMP

    def transform(step, carry):
        base = step * (count * CY)
        for n in range(count):
            tiles = []
            for y in range(8):
                f = curls[pl.ds(base + n * CY + (-y) % 8, 8, stride=8)]
                tiles.append(pltpu.roll(f, 16 * ((-y) % 8), 1) if y else f)
            for b in (1, 2, 4):
                moved = (granule & b) != 0
                tiles = [jnp.where(moved, tiles[(j - b) % 8], tiles[j]) for j in range(8)]
            for zb in range(8):
                tiled[zb * count * 8 + n * 8 : zb * count * 8 + n * 8 + 8] = tiles[zb]
        for zb in range(8):
            whole = tiled[zb * count * 8 : (zb + 1) * count * 8]
            high = whole.astype(jnp.bfloat16)
            low = (whole - high.astype(jnp.float32)).astype(jnp.bfloat16)
            both = jnp.dot(
                jnp.concatenate([high, low], axis=1),
                tables[zb * 256 : zb * 256 + 256],
                preferred_element_type=jnp.float32,
            )
            coeffs = both[:, :LANES] + both[:, LANES:]
            for n in range(count):
                p, c = n // COMP, n % COMP
                at = base + COMP * (p * CY + zb * 8) + c
                out[pl.ds(at, 8, stride=COMP)] = coeffs[n * 8 : n * 8 + 8]
        return carry

    lax.fori_loop(0, CX // PLANES, transform, 0)


def transform_of(curls):
    tables = jnp.asarray(tables_np())
    rows = COMP * NBLK
    return pl.pallas_call(
        transform_kernel,
        out_shape=jax.ShapeDtypeStruct((rows, LANES), jnp.float32),
        scratch_shapes=[pltpu.VMEM((PLANES * COMP * CY, LANES), jnp.float32)],
        cost_estimate=pl.CostEstimate(
            flops=2 * rows * 256 * 256, bytes_accessed=7_500_000, transcendentals=0
        ),
        compiler_params=pltpu.CompilerParams(vmem_limit_bytes=16 << 20),
        name="transform",
    )(curls, tables)


WIDTH = 4


def pack_kernel(rows, words, coeffs, head, one, two, three, four, out, room):
    lane = iota((COMP, LANES), 1)
    span, local_span = span_of(rows), room_of(rows)

    def body(r, carry):
        for j in range(WIDTH * LANES):
            p, yb, zb = j // CY, (j % CY) // 8, j % 8
            word = words[r * WIDTH + j // LANES, j % LANES]
            addr = word >> 7
            source = COMP * (p * CY + zb * 8 + yb)
            value = coeffs[pl.ds(r * (COMP * WIDTH * LANES) + source, COMP)]
            value = pltpu.roll(value, word, 1)
            kept = lane >= (jnp.full((COMP, LANES), word, jnp.int32) & (LANES - 1))
            pltpu.store(room.at[pl.ds(addr, COMP)], value, mask=kept)
            room[pl.ds(addr + COMP, COMP)] = value
        return carry

    lax.fori_loop(0, NBLK // LANES // WIDTH, body, 0)

    def settle(w, carry):
        for k in range(8):
            source = pl.multiple_of((w * 8 + k) * local_span, 8)
            target = pl.multiple_of((w * 8 + k) * span, 8)
            out[pl.ds(target, span)] = room[pl.ds(source, span)]
        return carry

    lax.fori_loop(0, WRITERS // 8, settle, 0)
    small = iota((8, LANES), 1)
    both = jnp.where(
        small == CAP,
        (one[...] + two[...]) + (three[...] + four[...]),
        jnp.maximum(jnp.maximum(one[...], two[...]), jnp.maximum(three[...], four[...])),
    )
    for w in range(0, WRITERS, 8):
        out[pl.ds(w * span + COMP * rows, 8, stride=span)] = jnp.where(
            small < CAP, head[w : w + 8], both
        )


def pack(words, coeffs, head, sums, rows):
    span = span_of(rows)
    return pl.pallas_call(
        functools.partial(pack_kernel, rows),
        in_specs=[
            pl.BlockSpec(memory_space=pltpu.SMEM),
            *[pl.BlockSpec(memory_space=pltpu.VMEM)] * 6,
        ],
        out_specs=pl.BlockSpec(memory_space=pltpu.VMEM),
        out_shape=jax.ShapeDtypeStruct((WRITERS * span, LANES), jnp.float32),
        scratch_shapes=[pltpu.VMEM((WRITERS * room_of(rows), LANES), jnp.float32)],
        cost_estimate=pl.CostEstimate(
            flops=200_000_000, bytes_accessed=8_000_000, transcendentals=0
        ),
        compiler_params=pltpu.CompilerParams(vmem_limit_bytes=22 << 20),
        name=f"pack{rows}",
    )(words, coeffs, head, *sums)


SOURCES = 8
ABREAST = 8


def unpack_kernel(rows, *refs):
    head = None
    if len(refs) == 10:
        head, refs = refs[0], refs[1:]
    recv, out, spill, heads, words_s, words_v, scale, pieces, sem = refs
    step = pl.program_id(0)
    span = span_of(rows)

    @pl.when(step == 0)
    def _():
        if head is None:
            h = recv[pl.ds(COMP * rows, WRITERS, stride=span)]
        else:
            h = head[...]
        heads[...] = h
        lane = iota((WRITERS, LANES), 1)
        lens = jnp.where(lane < CAP, h, 0.0)
        before = (iota((LANES, LANES), 0) < iota((LANES, LANES), 1)).astype(jnp.bfloat16)
        start = jnp.dot(lens.astype(jnp.bfloat16), before, preferred_element_type=jnp.float32)
        start = start.astype(jnp.int32)
        first = start >> 7
        turn = start & (LANES - 1)
        at = iota((WRITERS, LANES), 0) * span + COMP * jnp.minimum(first, rows - 2)
        late = (first >= rows - 1).astype(jnp.int32)
        words_v[...] = (
            (at << 17) + (lens.astype(jnp.int32) << 9) + (late << 8) + (LANES - turn)
        )
        copy = pltpu.make_async_copy(words_v, words_s, sem)
        copy.start()
        total = jnp.sum(jnp.where(lane == CAP, h, 0.0), keepdims=True)
        rms = jnp.sqrt(total * (1.0 / CELLS) + 1e-6)
        scale[...] = jnp.broadcast_to(1.0 / rms, scale.shape)
        spill[0, 0] = jnp.max(jnp.where(lane == CAP + 1, h, 0.0)).astype(jnp.int32)
        copy.wait()

    factor = scale[...]
    lane = iota((COMP, LANES), 1)

    def body(s, carry):
        for k in range(ABREAST * CAP):
            number, q = step * SOURCES + s * ABREAST + k // CAP, k % CAP
            word = words_s[number, q]
            marks = jnp.full((COMP, LANES), word, jnp.int32)
            at = word >> 17
            one = recv[pl.ds(at, COMP)]
            two = recv[pl.ds(at + COMP, COMP)]
            inside = ((marks & 511) + lane) & 384
            value = jnp.where(inside == LANES, one, two)
            value = pltpu.roll(value, word, 1)
            value = jnp.where(lane < ((marks >> 9) & 255), value, 0.0)
            pieces[k * 4 : k * 4 + COMP] = value
        for k in range(0, ABREAST * CAP, 8):
            for c in range(COMP):
                row = pl.multiple_of(s * (ABREAST * CAP) + k, 8)
                out[c, pl.ds(row, 8)] = pieces[pl.ds(k * 4 + c, 8, stride=4)] * factor
        return carry

    lax.fori_loop(0, SOURCES // ABREAST, body, 0)


def unpack(recv, rows, head=None):
    args = (recv,) if head is None else (head, recv)
    return pl.pallas_call(
        functools.partial(unpack_kernel, rows),
        grid=(WRITERS // SOURCES,),
        in_specs=[pl.BlockSpec(a.shape, lambda i: (0, 0)) for a in args],
        out_specs=[
            pl.BlockSpec((COMP, SOURCES * CAP, LANES), lambda i: (0, i, 0)),
            pl.BlockSpec(memory_space=pltpu.SMEM),
            pl.BlockSpec((WRITERS, LANES), lambda i: (0, 0)),
        ],
        out_shape=[
            jax.ShapeDtypeStruct((COMP, WRITERS * CAP, LANES), jnp.float32),
            jax.ShapeDtypeStruct((1, 1), jnp.int32),
            jax.ShapeDtypeStruct((WRITERS, LANES), jnp.float32),
        ],
        scratch_shapes=[
            pltpu.SMEM((WRITERS, LANES), jnp.int32),
            pltpu.VMEM((WRITERS, LANES), jnp.int32),
            pltpu.VMEM((8, LANES), jnp.float32),
            pltpu.VMEM((ABREAST * CAP * 4, LANES), jnp.float32),
            pltpu.SemaphoreType.DMA,
        ],
        cost_estimate=pl.CostEstimate(
            flops=200_000_000, bytes_accessed=11_000_000, transcendentals=0
        ),
        compiler_params=pltpu.CompilerParams(vmem_limit_bytes=24 << 20),
        name=f"unpack{rows}",
    )(*args)


def exchange(buffer, rows):
    return lax.all_to_all(
        buffer.reshape(WRITERS, span_of(rows), LANES), G, 0, 0, tiled=True
    )


def local(velocity, lengths, destinations):
    vel2 = velocity.reshape(COMP * CX * CY, LANES)
    mixed = (destinations * 256 + lengths.reshape(destinations.shape)).reshape(NBLK // LANES, LANES)

    xlo, xhi, ylo, yhi, zt, vel2 = faces(vel2)

    def ring(axis, n, d):
        return functools.partial(
            lax.ppermute, axis_name=axis, perm=[(i, (i + d) % n) for i in range(n)]
        )

    n_x, n_y, n_z = (lax.axis_size(a) for a in ("gx", "gy", "wa"))
    xprev, xnext = ring("gx", n_x, 1)(xhi), ring("gx", n_x, -1)(xlo)
    yprev, ynext = ring("gy", n_y, 1)(yhi), ring("gy", n_y, -1)(ylo)
    zprev, znext = ring("wa", n_z, 1)(zt), ring("wa", n_z, -1)(zt)
    words, wide, head = index(mixed)

    curls, mine = curl_of(vel2, xprev, xnext, yprev, ynext, zprev, znext, head)
    sums = [mine] + [ring("wa", n_z, d)(mine) for d in range(1, n_z)]
    coeffs = transform_of(curls)
    packed = pack(words, coeffs, head, sums, ROWS)
    got = exchange(packed, ROWS)
    out, spill, heads = unpack(got.reshape(-1, LANES), ROWS)

    def again(carry):
        more = exchange(pack(wide, coeffs, head, sums, CAP), CAP)
        wider, _, _ = unpack(more.reshape(-1, LANES), CAP, heads)
        return jnp.int32(0), wider

    _, out = lax.while_loop(lambda carry: carry[0] > 0, again, (spill.reshape(()), out))
    return out.reshape(1, 1, COMP, WRITERS, CAP, LANES)


def solution(mesh):
    return jax.shard_map(
        local,
        mesh=mesh,
        in_specs=(
            P(None, "gx", "gy", "wa"),
            P("gx", "gy", "wa", None),
            P("gx", "gy", "wa", None, None),
        ),
        out_specs=P(G, "wa", None, None, None, None),
        check_vma=False,
    )
```
